32 devices in a mesh: rep: 2 (over z, core), dp: 16 (over x, y).
Axes of the slice: x: 4, y: 4, z: 1, core: 2. Of those that a mesh axis runs over, the one named last changes fastest.
The devices are a block of a 4x4x8 slice.
Arguments:
- x: bfloat16 [32, 4096, 512], P(('rep', 'dp')), parts along dimension 0
- dy: bfloat16 [32, 4096, 512], P(('rep', 'dp')), parts along dimension 0
- w_gate: bfloat16 [2, 512, 1408], P(None, 'dp')
- w_up: bfloat16 [2, 512, 1408], P(None, 'dp')
- w_down: bfloat16 [2, 1408, 512], P(None, 'dp')
Outputs:
- output 1: bfloat16 [32, 4096, 512], P(('rep', 'dp')), parts along dimension 0
- output 2: bfloat16 [4, 512, 1408], P('rep', 'dp'), parts along dimension 0
- output 3: bfloat16 [4, 512, 1408], P('rep', 'dp'), parts along dimension 0
- output 4: bfloat16 [4, 1408, 512], P('rep', 'dp'), parts along dimension 0
There are 2 independent parts. The reference program is written for one: setup_inputs(seed, part) draws one part's arguments, and reference() takes and returns one part's arrays. A program takes and returns all parts, laid end to end along the dimension named above; an argument that names none is the same for every part.
All inputs are finite; a program needn't handle non-finite values.
Results may differ from the reference program's by a relative error of at most 0.018.
Values are sent between devices in bfloat16 or wider.
A program may use at most 768 MiB of HBM per device.

```python
import jax
import jax.numpy as jnp
from jax import lax

SEQUENCES = 16
TOKENS = 4096
D = 512
FF = 1408
LAYERS = 2
NAMES = ("w_gate", "w_up", "w_down")
SHAPES = {"w_gate": (LAYERS, D, FF), "w_up": (LAYERS, D, FF), "w_down": (LAYERS, FF, D)}


def bump(key, n, height):
    away = (jnp.arange(n, dtype=jnp.int32) - jax.random.randint(key, (), 0, n, jnp.int32)) % n
    return jnp.where(away < n // 8, height, 1.0)


def together(key, own, strength):
    shared = jax.random.normal(key, own.shape[1:], jnp.float32)
    return (own + strength * shared) * lax.rsqrt(1 + strength * strength)


def setup_inputs(seed: int = 0, part: int = 0) -> dict:
    kx, kdy, ka, kb, kz, kf, kh, kl, *kw = jax.random.split(jax.random.key(seed), 8 + len(NAMES))
    kx, kdy, ka, kb = (jax.random.fold_in(k, part) for k in (kx, kdy, ka, kb))
    shape = (SEQUENCES, TOKENS, D)
    much_x, much_dy = jax.random.uniform(kz, (2,), jnp.float32, 0.0, 1.0)
    layers = 2.0 ** jax.random.uniform(kl, (LAYERS, 1, 1), jnp.float32, -1.0, 1.0)
    x = together(ka, jax.random.normal(kx, shape, jnp.float32), much_x) * bump(kf, D, 4.0)
    dy = together(kb, jax.random.normal(kdy, shape, jnp.float32), much_dy)
    drawn = {"x": x.astype(jnp.bfloat16), "dy": (dy * (SEQUENCES * TOKENS) ** -0.5).astype(jnp.bfloat16)}
    for key, name in zip(kw, NAMES, strict=True):
        w = jax.random.normal(key, SHAPES[name], jnp.float32) * SHAPES[name][1] ** -0.5
        drawn[name] = (w * {"w_gate": 1.0, "w_up": bump(kh, FF, 4.0), "w_down": layers}[name]).astype(jnp.bfloat16)
    return drawn


def matmul(a, w):
    return jnp.dot(a, w, preferred_element_type=jnp.float32).astype(jnp.bfloat16)


def normed(h):
    wide = h.astype(jnp.float32)
    scale = lax.rsqrt(jnp.mean(wide**2, -1, keepdims=True) + 1e-6)
    return (wide * scale).astype(jnp.bfloat16)


def layer(h, w):
    a = normed(h)
    gate = jnp.dot(a, w["w_gate"], preferred_element_type=jnp.float32)
    up = jnp.dot(a, w["w_up"], preferred_element_type=jnp.float32)
    return h + matmul((jax.nn.silu(gate) * up).astype(jnp.bfloat16), w["w_down"])


def stack(weights, h):
    return lax.scan(lambda h, w: (layer(h, w), None), h, weights)[0]


def reference(x, dy, w_gate, w_up, w_down):
    weights = dict(zip(NAMES, (w_gate, w_up, w_down), strict=True))

    def take(so_far, sequence):
        h, by_y = sequence
        _, back = jax.vjp(stack, weights, h)
        by_weights, by_h = back(by_y)
        return jax.tree.map(lambda total, term: total + term.astype(jnp.float32), so_far, by_weights), by_h

    none_yet = {name: jnp.zeros(w.shape, jnp.float32) for name, w in weights.items()}
    by_weights, by_x = lax.scan(take, none_yet, (x, dy))
    return (by_x, *(by_weights[name].astype(jnp.bfloat16) for name in NAMES))
```

```python
import functools
import math

import jax
import jax.numpy as jnp
from jax import lax
from jax.experimental import pallas as pl
from jax.experimental.pallas import tpu as pltpu
from jax.sharding import PartitionSpec as P

bf16, f32 = jnp.bfloat16, jnp.float32
MESH = pl.DeviceIdType.MESH
TILE = 512
CHUNK = 256
STEPS = 4
DIMS = ((1, 0), (0, 1), (3, 0), (0, 3))


def dot(a, b):
    return jnp.dot(a, b, preferred_element_type=f32)


def dot_t(a, b):
    return lax.dot_general(a, b, (((0,), (0,)), ((), ())), preferred_element_type=f32)


def flip(c, bits):
    return (c, c + 1 - 2 * lax.rem(c, 2), lax.rem(c + 2, 4), 3 - c)[bits]


def mask_of(part, slot):
    x = y = 0
    for bit in range(STEPS):
        if slot >> bit & 1:
            dx, dy = DIMS[(part + STEPS - 1 - bit) % 4]
            x, y = x ^ dx, y ^ dy
    return x, y


def kernel(sizes, x_hbm, dy_hbm, wg_ref, wu_ref, wd_ref, dx_hbm, og_ref, ou_ref, od_ref, *scratch):
    (x_s, h_s, dy_s, wgu, wd0, wgut, wdt, acc_gu, acc_d, p_s, dgu_s, *rest) = scratch
    slots = (rest[:8], rest[8:16])
    send_sem, recv_sem, credit, copy_sem, out_sem = rest[16:]
    tokens, width, hidden, deep, share_gu, share_d = sizes
    me = lax.axis_index("dp")
    mx, my = lax.div(me, 4), lax.rem(me, 4)

    def device(mask):
        return flip(mx, mask[0]) * 4 + flip(my, mask[1])

    lanes = 2 * hidden // 128
    cuts = [128 * (lanes * q // 4) for q in range(5)]
    cols_gu = list(zip(cuts, cuts[1:]))
    cols_d = [(width * q // 4, width * (q + 1) // 4) for q in range(4)]
    cols = cols_gu + cols_d

    copies = [pltpu.make_async_copy(x_hbm, x_s, copy_sem.at[0]), pltpu.make_async_copy(dy_hbm, dy_s, copy_sem.at[1])]
    for copy in copies:
        copy.start()

    barrier = pltpu.get_barrier_semaphore()
    for dim in DIMS:
        pl.semaphore_signal(barrier, inc=1, device_id={"dp": device(dim)}, device_id_type=MESH)

    def gate_up(ref_g, ref_u, layer, lo, hi):
        pieces = []
        if lo < hidden:
            pieces.append(ref_g[layer, :, lo:min(hi, hidden)])
        if hi > hidden:
            pieces.append(ref_u[layer, :, max(lo, hidden) - hidden:hi - hidden])
        return pieces

    def own_blocks(layer):
        for q, (lo, hi) in enumerate(cols_gu):
            at = 0
            for piece in gate_up(wg_ref, wu_ref, layer, lo, hi):
                slots[layer][q][0, :, at:at + piece.shape[1]] = piece
                at += piece.shape[1]
        for q, (lo, hi) in enumerate(cols_d):
            slots[layer][4 + q][0] = wd_ref[layer, :, lo:hi]

    def gather_copy(layer, step, a):
        q, n = a % 4, 2**step
        return pltpu.make_async_remote_copy(
            src_ref=slots[layer][a].at[pl.ds(0, n)], dst_ref=slots[layer][a].at[pl.ds(n, n)],
            send_sem=send_sem.at[layer, a, step], recv_sem=recv_sem.at[layer, a, step],
            device_id={"dp": device(DIMS[(q + STEPS - 1 - step) % 4])}, device_id_type=MESH)

    def gather_start(layer, step):
        for a in range(8):
            gather_copy(layer, step, a).start()

    def gather_wait(layer, step):
        for a in range(8):
            gather_copy(layer, step, a).wait()

    def install(layer):
        for r in range(16):
            for a, (lo, hi) in enumerate(cols):
                owner = device(mask_of(a % 4, r))
                if a < 4:
                    wgu[layer, pl.ds(pl.multiple_of(owner * share_gu, share_gu), share_gu), lo:hi] = slots[layer][a][r]
                else:
                    acc_d[layer, pl.ds(pl.multiple_of(owner * share_d, 8), share_d), lo:hi] = slots[layer][a][r].astype(f32)

    def scatter_copy(layer, step, a):
        q, n = a % 4, 2 ** (STEPS - 1 - step)
        return pltpu.make_async_remote_copy(
            src_ref=slots[1][a].at[pl.ds(n, n)], dst_ref=slots[0][a].at[pl.ds(n, n)],
            send_sem=send_sem.at[2 + layer, a, step], recv_sem=recv_sem.at[2 + layer, a, step],
            device_id={"dp": device(DIMS[(q + step) % 4])}, device_id_type=MESH)

    def scatter_start(layer, step):
        for a in range(8):
            if layer == 0:
                pl.semaphore_wait(credit.at[a, step], 1)
            scatter_copy(layer, step, a).start()

    def scatter_fill(layer):
        for r in range(8, 16):
            for a, (lo, hi) in enumerate(cols):
                acc, share = (acc_gu, share_gu) if a < 4 else (acc_d, share_d)
                owner = device(mask_of(a % 4, r))
                slots[1][a][r] = acc[layer, pl.ds(pl.multiple_of(owner * share, 8), share), lo:hi].astype(bf16)

    def scatter_add(layer, step):
        n = 2 ** (STEPS - 1 - step)
        for a, (lo, hi) in enumerate(cols):
            scatter_copy(layer, step, a).wait()
            acc, share = (acc_gu, share_gu) if a < 4 else (acc_d, share_d)
            for r in range(n):
                rows = pl.ds(pl.multiple_of(device(mask_of(a % 4, r)) * share, 8), share)
                total = acc[layer, rows, lo:hi] + slots[0][a][n + r].astype(f32)
                if n == 1:
                    total = total.astype(bf16)
                    if a >= 4:
                        od_ref[layer, :, lo:hi] = total
                    else:
                        if lo < hidden:
                            og_ref[layer, :, lo:min(hi, hidden)] = total[:, :min(hi, hidden) - lo]
                        if hi > hidden:
                            ou_ref[layer, :, max(lo, hidden) - hidden:hi - hidden] = total[:, max(lo, hidden) - lo:]
                elif r >= n // 2:
                    slots[1][a][r] = total.astype(bf16)
                else:
                    acc[layer, rows, lo:hi] = total
            if layer == 1:
                pl.semaphore_signal(credit.at[a, step], inc=1, device_id={"dp": device(DIMS[(a + step) % 4])}, device_id_type=MESH)

    chunks = [(lo, min(lo + CHUNK, hidden)) for lo in range(0, hidden, CHUNK)]

    def normed(ref, rows):
        wide = ref[rows, :].astype(f32)
        scale = lax.rsqrt(jnp.mean(wide * wide, -1, keepdims=True) + 1e-6)
        return wide, scale, (wide * scale).astype(bf16)

    def at_tile(i):
        return pl.ds(pl.multiple_of(i * TILE, TILE), TILE)

    def transposes(layer, down):
        for lo in range(0, 2 * hidden, CHUNK):
            wgut[lo:lo + CHUNK, :] = wgu[layer, :, lo:lo + CHUNK].T
        for lo, hi in chunks:
            wdt[:, lo:hi] = down[lo:hi, :].T.astype(bf16)

    def backward(layer, i, h_ref, dy_ref, out_ref):
        rows = at_tile(i)
        wide, scale, a = normed(h_ref, rows)
        dy = dy_ref[rows, :]
        for lo, hi in chunks:
            g, u = dot(a, wgu[layer, :, lo:hi]), dot(a, wgu[layer, :, hidden + lo:hidden + hi])
            dq = dot(dy, wdt[:, lo:hi]).astype(bf16).astype(f32)
            sig = 0.5 * jnp.tanh(0.5 * g) + 0.5
            s = g * sig
            p_s[:, lo:hi] = (s * u).astype(bf16)
            dgu_s[:, hidden + lo:hidden + hi] = (dq * s).astype(bf16)
            dgu_s[:, lo:hi] = (dq * u * (sig + s * (1 - sig))).astype(bf16)
        acc_d[layer] += dot_t(p_s[...], dy)
        acc_gu[layer] += dot_t(a, dgu_s[...])
        da = dot(dgu_s[...], wgut[...]).astype(bf16).astype(f32)
        mean = jnp.mean(da * wide, -1, keepdims=True)
        out_ref[rows, :] = dy + (da * scale - wide * (mean * scale * scale * scale)).astype(bf16)

    own_blocks(0)
    own_blocks(1)
    pl.semaphore_wait(barrier, 4)
    for step in range(STEPS):
        gather_start(0, step)
        gather_wait(0, step)
    gather_start(1, 0)
    install(0)
    wd0[...] = acc_d[0].astype(bf16)
    for copy in copies:
        copy.wait()

    def forward(i, _):
        for step, when in enumerate((2, 4, 7)):
            @pl.when(i == when)
            def _():
                gather_wait(1, step)
                gather_start(1, step + 1)
        rows = at_tile(i)
        _, _, a = normed(x_s, rows)
        for lo, hi in chunks:
            g, u = dot(a, wgu[0, :, lo:hi]), dot(a, wgu[0, :, hidden + lo:hidden + hi])
            p_s[:, lo:hi] = (g * (0.5 * jnp.tanh(0.5 * g) + 0.5) * u).astype(bf16)
        h_s[rows, :] = x_s[rows, :] + dot(p_s[...], wd0[...]).astype(bf16)
        return 0

    tiles = tokens // TILE
    lax.fori_loop(0, tiles, forward, 0)
    gather_wait(1, STEPS - 1)
    install(1)
    transposes(1, acc_d.at[1])
    acc_gu[...] = jnp.zeros_like(acc_gu)
    acc_d[...] = jnp.zeros_like(acc_d)

    def last(i, _):
        backward(1, i, h_s, dy_s, h_s)
        return 0

    lax.fori_loop(0, tiles, last, 0)
    scatter_fill(1)
    scatter_start(1, 0)
    transposes(0, wd0)

    def out_copy(i):
        return pltpu.make_async_copy(x_s.at[at_tile(i)], dx_hbm.at[at_tile(i)], out_sem.at[i])

    def first(i, _):
        for step, when in enumerate((2, 4, 5, 6)):
            @pl.when(i == when)
            def _():
                scatter_add(1, step)
                if step < STEPS - 1:
                    scatter_start(1, step + 1)
        backward(0, i, x_s, h_s, x_s)
        out_copy(i).start()
        return 0

    lax.fori_loop(0, tiles, first, 0)
    scatter_fill(0)
    for step in range(STEPS):
        scatter_start(0, step)
        scatter_add(0, step)
    for i in range(tiles):
        out_copy(i).wait()


def solution(mesh):
    group = mesh.shape["dp"]
    side = math.isqrt(group)
    assert side * side == group == 2**STEPS

    def local(x, dy, w_gate, w_up, w_down):
        _, tokens, width = x.shape
        layers, share_gu, hidden = w_gate.shape
        share_d = w_down.shape[1]
        lanes = 2 * hidden // 128
        cuts = [128 * (lanes * q // 4) for q in range(5)]
        parts = [pltpu.VMEM((group, share_gu, hi - lo), bf16) for lo, hi in zip(cuts, cuts[1:])]
        parts += [pltpu.VMEM((group, share_d, width // 4), bf16)] * 4
        any_, vmem = pl.BlockSpec(memory_space=pl.ANY), pl.BlockSpec(memory_space=pltpu.VMEM)
        out = pl.pallas_call(
            functools.partial(kernel, (tokens, width, hidden, layers, share_gu, share_d)),
            out_shape=[jax.ShapeDtypeStruct(s, bf16) for s in ((tokens, width), w_gate.shape, w_up.shape, w_down.shape)],
            in_specs=[any_, any_, vmem, vmem, vmem],
            out_specs=[any_, vmem, vmem, vmem],
            scratch_shapes=[pltpu.VMEM((tokens, width), bf16)] * 3 + [
                pltpu.VMEM((layers, width, 2 * hidden), bf16),
                pltpu.VMEM((hidden, width), bf16),
                pltpu.VMEM((2 * hidden, width), bf16),
                pltpu.VMEM((width, hidden), bf16),
                pltpu.VMEM((layers, width, 2 * hidden), f32),
                pltpu.VMEM((layers, hidden, width), f32),
                pltpu.VMEM((TILE, hidden), bf16),
                pltpu.VMEM((TILE, 2 * hidden), bf16),
            ] + parts * 2 + [
                pltpu.SemaphoreType.DMA((4, 8, STEPS)),
                pltpu.SemaphoreType.DMA((4, 8, STEPS)),
                pltpu.SemaphoreType.REGULAR((8, STEPS)),
                pltpu.SemaphoreType.DMA((2,)),
                pltpu.SemaphoreType.DMA((tokens // TILE,)),
            ],
            compiler_params=pltpu.CompilerParams(collective_id=0, has_side_effects=True, vmem_limit_bytes=67043328),
            name="stack",
        )(x[0], dy[0], w_gate, w_up, w_down)
        return (out[0][None], *out[1:])

    tokens_spec = P(("rep", "dp"), None, None)
    weight_spec, grad_spec = P(None, "dp", None), P("rep", "dp", None)
    return jax.shard_map(local, mesh=mesh, in_specs=(tokens_spec, tokens_spec) + (weight_spec,) * 3,
                         out_specs=(tokens_spec,) + (grad_spec,) * 3, check_vma=False)
```

```python
import functools
import math

import jax
import jax.numpy as jnp
from jax import lax
from jax.experimental import pallas as pl
from jax.experimental.pallas import tpu as pltpu
from jax.sharding import PartitionSpec as P

bf16, f32 = jnp.bfloat16, jnp.float32
MESH = pl.DeviceIdType.MESH
TILE = 512
CHUNK = 256
STEPS = 4
DIMS = ((1, 0), (0, 1), (3, 0), (0, 3))
PART = (0, 1, 0, 1, 2, 3, 2, 3, 0, 1, 2, 3)


def dot(a, b):
    return jnp.dot(a, b, preferred_element_type=f32)


def dot_t(a, b):
    return lax.dot_general(a, b, (((0,), (0,)), ((), ())), preferred_element_type=f32)


def flip(c, bits):
    return (c, c + 1 - 2 * lax.rem(c, 2), lax.rem(c + 2, 4), 3 - c)[bits]


def mask_of(part, slot):
    x = y = 0
    for bit in range(STEPS):
        if slot >> bit & 1:
            dx, dy = DIMS[(part + STEPS - 1 - bit) % 4]
            x, y = x ^ dx, y ^ dy
    return x, y


def kernel(sizes, x_hbm, dy_hbm, wg_ref, wu_ref, wd_ref, dx_hbm, og_ref, ou_ref, od_ref, p_hbm, dgu_hbm, *scratch):
    (x_s, h_s, dy_s, wgu, wd0, wgut, wdt, acc_gu, acc_d, p_s, dgu_s, *rest) = scratch
    slots = (rest[:12], rest[12:24])
    send_sem, recv_sem, hand_send, hand_recv, credit, copy_sem, out_sem, p_sem, dgu_sem = rest[24:]
    tokens, width, hidden, share_gu, share_d = sizes
    me, rep = lax.axis_index("dp"), lax.axis_index("rep")
    mx, my = lax.div(me, 4), lax.rem(me, 4)
    core = lax.rem(rep, 2)
    tiles = tokens // TILE

    def device(mask):
        return flip(mx, mask[0]) * 4 + flip(my, mask[1])

    def to(dim):
        return {"dp": device(DIMS[dim % 4])}

    partner = {"rep": rep + 1 - 2 * core}
    pieces = pieces_of(hidden)
    cols = pieces + [(hidden + lo, hidden + hi) for lo, hi in pieces] + [(width * q // 4, width * (q + 1) // 4) for q in range(4)]
    GU, D = range(8), range(8, 12)
    half = pieces[2][0]
    FIRST, SECOND = (0, 1, 4, 5), (2, 3, 6, 7)
    keeper = (0, 0, 0, 0, 1, 1, 1, 1, 0, 0, 1, 1)

    copies = [pltpu.make_async_copy(x_hbm, x_s, copy_sem.at[0]), pltpu.make_async_copy(dy_hbm, dy_s, copy_sem.at[1])]
    for copy in copies:
        copy.start()

    barrier = pltpu.get_barrier_semaphore()
    for peer in [to(dim) for dim in range(4)] + [partner]:
        pl.semaphore_signal(barrier, inc=1, device_id=peer, device_id_type=MESH)

    def rows_of(a, slot):
        share = share_gu if a < 8 else share_d
        return pl.ds(pl.multiple_of(device(mask_of(PART[a], slot)) * share, 8), share)

    def own_blocks(layer):
        for a, (lo, hi) in enumerate(cols):
            if a < 4:
                slots[layer][a][0] = wg_ref[layer, :, lo:hi]
            elif a < 8:
                slots[layer][a][0] = wu_ref[layer, :, lo - hidden:hi - hidden]
            else:
                slots[layer][a][0] = wd_ref[layer, :, lo:hi]

    def gather_copy(layer, step, a):
        n = 2**step
        return pltpu.make_async_remote_copy(
            src_ref=slots[layer][a].at[pl.ds(0, n)], dst_ref=slots[layer][a].at[pl.ds(n, n)],
            send_sem=send_sem.at[layer, a, step], recv_sem=recv_sem.at[layer, a, step],
            device_id=to(PART[a] + STEPS - 1 - step), device_id_type=MESH)

    def hand_copy(layer, step, a):
        there = slots[layer][a].at[pl.ds(2**step, 2**step)]
        return pltpu.make_async_remote_copy(
            src_ref=there, dst_ref=there, send_sem=hand_send.at[layer, a, step], recv_sem=hand_recv.at[layer, a, step],
            device_id=partner, device_id_type=MESH)

    def by_core(arrays, act):
        for side in range(2):
            @pl.when(core == side)
            def _():
                act([a for a in arrays if keeper[a] == side], [a for a in arrays if keeper[a] != side])

    def gather_step(layer, step, arrays, then=None):
        def act(mine, _):
            for a in mine:
                if step > 0:
                    gather_copy(layer, step - 1, a).wait()
                if step < STEPS:
                    gather_copy(layer, step, a).start()
                if step > 0:
                    hand_copy(layer, step - 1, a).start()
        by_core(arrays, act)

    def gather_end(layer, arrays):
        def act(mine, others):
            for step in range(STEPS):
                for a in others:
                    hand_copy(layer, step, a).wait_recv()
                for a in mine:
                    hand_copy(layer, step, a).wait_send()
        by_core(arrays, act)

    def install(layer, arrays):
        for r in range(16):
            for a in arrays:
                lo, hi = cols[a]
                if a < 8:
                    wgu[layer, rows_of(a, r), lo:hi] = slots[layer][a][r]
                else:
                    acc_d[layer, rows_of(a, r), lo:hi] = slots[layer][a][r].astype(f32)

    def scatter_copy(layer, step, a):
        n = 2 ** (STEPS - 1 - step)
        return pltpu.make_async_remote_copy(
            src_ref=slots[1][a].at[pl.ds(n, n)], dst_ref=slots[0][a].at[pl.ds(n, n)],
            send_sem=send_sem.at[2 + layer, a, step], recv_sem=recv_sem.at[2 + layer, a, step],
            device_id=to(PART[a] + step), device_id_type=MESH)

    def scatter_start(layer, step, arrays):
        for a in arrays:
            if layer == 0:
                pl.semaphore_wait(credit.at[a, step], 1)
            scatter_copy(layer, step, a).start()

    def scatter_fill(layer, arrays):
        for a in arrays:
            lo, hi = cols[a]
            acc = acc_gu if a < 8 else acc_d
            for r in range(8, 16):
                slots[1][a][r] = acc[layer, rows_of(a, r), lo:hi].astype(bf16)
        scatter_start(layer, 0, arrays)

    def scatter_add(layer, step, arrays):
        n = 2 ** (STEPS - 1 - step)
        for a in arrays:
            lo, hi = cols[a]
            scatter_copy(layer, step, a).wait()
            acc = acc_gu if a < 8 else acc_d
            for r in reversed(range(n)):
                total = acc[layer, rows_of(a, r), lo:hi] + slots[0][a][n + r].astype(f32)
                if n == 1:
                    if a < 4:
                        og_ref[layer, :, lo:hi] = total.astype(bf16)
                    elif a < 8:
                        ou_ref[layer, :, lo - hidden:hi - hidden] = total.astype(bf16)
                    else:
                        od_ref[layer, :, lo:hi] = total.astype(bf16)
                elif r >= n // 2:
                    slots[1][a][r] = total.astype(bf16)
                else:
                    acc[layer, rows_of(a, r), lo:hi] = total
            if layer == 1:
                pl.semaphore_signal(credit.at[a, step], inc=1, device_id=to(PART[a] + step), device_id_type=MESH)
        if step < STEPS - 1:
            scatter_start(layer, step + 1, arrays)

    def chunks_of(lo, hi):
        return [(at, min(at + CHUNK, hi)) for at in range(lo, hi, CHUNK)]

    def normed(ref, rows):
        wide = ref[rows, :].astype(f32)
        scale = lax.rsqrt(jnp.mean(wide * wide, -1, keepdims=True) + 1e-6)
        return wide, scale, (wide * scale).astype(bf16)

    def at_tile(i):
        return pl.ds(pl.multiple_of(i * TILE, TILE), TILE)

    def loop(events, body):
        def step(i, _):
            for when, actions in events.items():
                @pl.when(i == when)
                def _():
                    for act, *args in actions:
                        act(*args)
            body(i)
            return 0
        lax.fori_loop(0, tiles, step, 0)

    def transposes(layer, down):
        for lo in range(0, 2 * hidden, CHUNK):
            wgut[lo:lo + CHUNK, :] = wgu[layer, :, lo:lo + CHUNK].T
        for lo, hi in chunks_of(0, hidden):
            wdt[:, lo:hi] = down[lo:hi, :].T.astype(bf16)

    def inner(layer, a, dy, span, dgu_ref, p_ref=None):
        for lo, hi in chunks_of(*span):
            g, u = dot(a, wgu[layer, :, lo:hi]), dot(a, wgu[layer, :, hidden + lo:hidden + hi])
            dq = dot(dy, wdt[:, lo:hi]).astype(bf16).astype(f32)
            sig = 0.5 * jnp.tanh(0.5 * g) + 0.5
            s = g * sig
            if p_ref is not None:
                p_ref[:, lo:hi] = (s * u).astype(bf16)
            dgu_ref[:, hidden + lo:hidden + hi] = (dq * s).astype(bf16)
            dgu_ref[:, lo:hi] = (dq * u * (sig + s * (1 - sig))).astype(bf16)

    def outer(wide, scale, dy, dgu_ref):
        da = dot(dgu_ref[...], wgut[...]).astype(bf16).astype(f32)
        mean = jnp.mean(da * wide, -1, keepdims=True)
        return dy + (da * scale - wide * (mean * scale * scale * scale)).astype(bf16)

    own_blocks(0)
    own_blocks(1)
    pl.semaphore_wait(barrier, 5)
    gather_step(0, 0, GU)
    gather_step(0, 0, D)
    gather_step(0, 1, GU)
    gather_step(0, 1, D)
    gather_step(0, 2, GU)
    gather_step(0, 2, D)
    gather_step(0, 3, GU)
    gather_step(0, 3, D)
    gather_step(1, 0, range(12))
    acc_gu[...] = jnp.zeros_like(acc_gu)
    gather_step(0, 4, GU)
    gather_end(0, GU)
    install(0, GU)
    for copy in copies:
        copy.wait()

    def p_copy(i, out):
        there, here = p_hbm.at[at_tile(i)], p_s.at[lax.rem(i, 2)]
        return pltpu.make_async_copy(*((here, there) if out else (there, here)), p_sem.at[lax.rem(i, 2)])

    def forward(i):
        rows = at_tile(i)
        slot = lax.rem(i, 2)
        _, _, a = normed(x_s, rows)

        @pl.when(i >= 2)
        def _():
            p_copy(i - 2, True).wait()
        for lo, hi in chunks_of(0, hidden):
            g, u = dot(a, wgu[0, :, lo:hi]), dot(a, wgu[0, :, hidden + lo:hidden + hi])
            p_s[slot, :, lo:hi] = (g * (0.5 * jnp.tanh(0.5 * g) + 0.5) * u).astype(bf16)
        p_copy(i, True).start()

        @pl.when(i == 0)
        def _():
            gather_step(0, 4, D)
            gather_end(0, D)
            install(0, D)
            wd0[...] = acc_d[0].astype(bf16)
        h_s[rows, :] = x_s[rows, :] + dot(p_s[slot], wd0[...]).astype(bf16)

    every = range(12)
    loop({1: [(gather_step, 1, 1, every)], 2: [(gather_step, 1, 2, every)], 4: [(gather_step, 1, 3, every)], 7: [(gather_step, 1, 4, every)]}, forward)
    p_copy(tiles - 2, True).wait()
    p_copy(tiles - 1, True).wait()
    gather_end(1, every)
    install(1, every)
    transposes(1, acc_d.at[1])
    acc_d[...] = jnp.zeros_like(acc_d)

    def last(i):
        rows = at_tile(i)
        wide, scale, a = normed(h_s, rows)
        dy = dy_s[rows, :]
        inner(1, a, dy, (0, hidden), dgu_s.at[0], p_s.at[0])
        acc_d[1] += dot_t(p_s[0], dy)
        acc_gu[1] += dot_t(a, dgu_s[0])
        h_s[rows, :] = outer(wide, scale, dy, dgu_s.at[0])

    loop({}, last)
    p_copy(0, False).start()
    scatter_fill(1, every)
    transposes(0, wd0)

    def down(i):
        slot = lax.rem(i, 2)

        @pl.when(i < tiles - 1)
        def _():
            p_copy(i + 1, False).start()
        p_copy(i, False).wait()
        acc_d[0] += dot_t(p_s[slot], h_s[at_tile(i), :])

    def dgu_copies(i, span, out):
        slot = lax.rem(i, 2)
        found = []
        for side in range(2):
            place = pl.ds(side * hidden + span[0], span[1] - span[0])
            there, here = dgu_hbm.at[at_tile(i), place], dgu_s.at[slot, :, place]
            found.append(pltpu.make_async_copy(*((here, there) if out else (there, here)), dgu_sem.at[slot, side]))
        return found

    def gate_up(i, span):
        slot = lax.rem(i, 2)
        rows = at_tile(i)
        _, _, a = normed(x_s, rows)

        @pl.when(i >= 2)
        def _():
            for copy in dgu_copies(i - 2, span, True):
                copy.wait()
        inner(0, a, h_s[rows, :], span, dgu_s.at[slot])
        for copy in dgu_copies(i, span, True):
            copy.start()
        for side in range(2):
            lo, hi = (side * hidden + at for at in span)
            acc_gu[0, :, lo:hi] += dot_t(a, dgu_s[slot, :, lo:hi])

    def drain(span):
        for i in range(tiles - 2, tiles):
            for copy in dgu_copies(i, span, True):
                copy.wait()

    def out_copy(i):
        return pltpu.make_async_copy(x_s.at[at_tile(i)], dx_hbm.at[at_tile(i)], out_sem.at[i])

    def back(i):
        slot = lax.rem(i, 2)
        whole = (0, hidden)
        rows = at_tile(i)

        @pl.when(i < tiles - 1)
        def _():
            for copy in dgu_copies(i + 1, whole, False):
                copy.start()
        for copy in dgu_copies(i, whole, False):
            copy.wait()
        wide, scale, _ = normed(x_s, rows)
        x_s[rows, :] = outer(wide, scale, h_s[rows, :], dgu_s.at[slot])
        out_copy(i).start()

    loop({}, down)
    loop({2: [(scatter_add, 1, 0, every), (scatter_fill, 0, D)], 4: [(scatter_add, 1, 1, every)], 5: [(scatter_add, 0, 0, D), (scatter_add, 1, 2, every)],
          6: [(scatter_add, 0, 1, D)], 7: [(scatter_add, 1, 3, every), (scatter_add, 0, 2, D)]}, lambda i: gate_up(i, (0, half)))
    drain((0, half))
    scatter_fill(0, FIRST)
    loop({1: [(scatter_add, 0, 3, D)], 3: [(scatter_add, 0, 0, FIRST)], 5: [(scatter_add, 0, 1, FIRST)], 7: [(scatter_add, 0, 2, FIRST)]},
         lambda i: gate_up(i, (half, hidden)))
    drain((half, hidden))
    for copy in dgu_copies(0, (0, hidden), False):
        copy.start()
    scatter_fill(0, SECOND)
    loop({0: [(scatter_add, 0, 3, FIRST)], 3: [(scatter_add, 0, 0, SECOND)], 5: [(scatter_add, 0, 1, SECOND)], 7: [(scatter_add, 0, 2, SECOND)]}, back)
    scatter_add(0, 3, SECOND)
    for i in range(tiles):
        out_copy(i).wait()


def pieces_of(hidden):
    lanes = hidden // 128
    cuts = [128 * -(-lanes * q // 4) for q in range(5)]
    return list(zip(cuts, cuts[1:]))


def solution(mesh):
    group = mesh.shape["dp"]
    side = math.isqrt(group)
    assert side * side == group == 2**STEPS

    def local(x, dy, w_gate, w_up, w_down):
        _, tokens, width = x.shape
        layers, share_gu, hidden = w_gate.shape
        share_d = w_down.shape[1]
        parts = [pltpu.VMEM((group, share_gu, hi - lo), bf16) for lo, hi in pieces_of(hidden) * 2]
        parts += [pltpu.VMEM((group, share_d, width // 4), bf16)] * 4
        any_, vmem = pl.BlockSpec(memory_space=pl.ANY), pl.BlockSpec(memory_space=pltpu.VMEM)
        shapes = ((tokens, width), w_gate.shape, w_up.shape, w_down.shape, (tokens, hidden), (tokens, 2 * hidden))
        dma, tiles = pltpu.SemaphoreType.DMA, tokens // TILE
        out = pl.pallas_call(
            functools.partial(kernel, (tokens, width, hidden, share_gu, share_d)),
            out_shape=[jax.ShapeDtypeStruct(s, bf16) for s in shapes],
            in_specs=[any_, any_, vmem, vmem, vmem],
            out_specs=[any_, vmem, vmem, vmem, any_, any_],
            scratch_shapes=[pltpu.VMEM((tokens, width), bf16)] * 3 + [
                pltpu.VMEM((layers, width, 2 * hidden), bf16),
                pltpu.VMEM((hidden, width), bf16),
                pltpu.VMEM((2 * hidden, width), bf16),
                pltpu.VMEM((width, hidden), bf16),
                pltpu.VMEM((layers, width, 2 * hidden), f32),
                pltpu.VMEM((layers, hidden, width), f32),
                pltpu.VMEM((2, TILE, hidden), bf16),
                pltpu.VMEM((2, TILE, 2 * hidden), bf16),
            ] + parts * 2 + [
                dma((4, 12, STEPS)), dma((4, 12, STEPS)), dma((2, 12, STEPS)), dma((2, 12, STEPS)),
                pltpu.SemaphoreType.REGULAR((12, STEPS)), dma((2,)), dma((tiles,)), dma((2,)), dma((2, 2)),
            ],
            compiler_params=pltpu.CompilerParams(collective_id=0, has_side_effects=True, vmem_limit_bytes=67043328),
            name="stack",
        )(x[0], dy[0], w_gate, w_up, w_down)
        return (out[0][None], *out[1:4])

    tokens_spec = P(("rep", "dp"), None, None)
    weight_spec, grad_spec = P(None, "dp", None), P("rep", "dp", None)
    return jax.shard_map(local, mesh=mesh, in_specs=(tokens_spec, tokens_spec) + (weight_spec,) * 3,
                         out_specs=(tokens_spec,) + (grad_spec,) * 3, check_vma=False)
```

```python
import functools
import math

import jax
import jax.numpy as jnp
from jax import lax
from jax.experimental import pallas as pl
from jax.experimental.pallas import tpu as pltpu
from jax.sharding import PartitionSpec as P

bf16, f32 = jnp.bfloat16, jnp.float32
MESH = pl.DeviceIdType.MESH
TILE = 512
CHUNK = 256
STEPS = 4
VMEM_LIMIT = 67043328
DIMS = ((1, 0), (0, 1), (3, 0), (0, 3))
PART = (0, 1, 0, 1, 2, 3, 2, 3, 0, 1, 2, 3)


def dot(a, b):
    return jnp.dot(a, b, preferred_element_type=f32)


def dot_t(a, b):
    return lax.dot_general(a, b, (((0,), (0,)), ((), ())), preferred_element_type=f32)


def flip(c, bits):
    return (c, c + 1 - 2 * lax.rem(c, 2), lax.rem(c + 2, 4), 3 - c)[bits]


def mask_of(part, slot):
    x = y = 0
    for bit in range(STEPS):
        if slot >> bit & 1:
            dx, dy = DIMS[(part + STEPS - 1 - bit) % 4]
            x, y = x ^ dx, y ^ dy
    return x, y


def kernel(sizes, x_hbm, dy_hbm, wg_hbm, wu_hbm, wd_hbm, h_s, og_hbm, ou_hbm, od_hbm, p_hbm, dgu_hbm, a_hbm, gu_hbm, *scratch):
    (in_s, gu_s, wgu, wgut, wdt, acc_gu, acc_d, p_s, dgu_s, *rest) = scratch
    slots = (rest[:12], rest[12:24])
    send_sem, recv_sem, hand_send, hand_recv, credit, own_sem, in_sem, a_sem, p_sem, dgu_sem, gu_sem = rest[24:]
    tokens, width, hidden, share_gu, share_d = sizes
    a_s = dgu_s.at[:, :, :width]
    wd0 = [(lo, min(lo + TILE, hidden), dgu_s.at[1, :min(TILE, hidden - lo), pl.ds((1 + lo // TILE) * width, width)]) for lo in range(0, hidden, TILE)]
    me, rep = lax.axis_index("dp"), lax.axis_index("rep")
    mx, my = lax.div(me, 4), lax.rem(me, 4)
    core = lax.rem(rep, 2)
    tiles = tokens // TILE

    def device(mask):
        return flip(mx, mask[0]) * 4 + flip(my, mask[1])

    def to(dim):
        return {"dp": device(DIMS[dim % 4])}

    partner = {"rep": rep + 1 - 2 * core}
    pieces = pieces_of(hidden)
    cols = pieces + [(hidden + lo, hidden + hi) for lo, hi in pieces] + [(width * q // 4, width * (q + 1) // 4) for q in range(4)]
    GU, D = range(8), range(8, 12)
    half = pieces[2][0]
    FIRST, SECOND = (0, 1, 4, 5), (2, 3, 6, 7)
    keeper = (0, 0, 0, 0, 1, 1, 1, 1, 0, 0, 1, 1)

    def in_copy(source, i):
        return pltpu.make_async_copy(source.at[at_tile(i)], in_s.at[lax.rem(i, 2)], in_sem.at[lax.rem(i, 2)])

    def streamed(source, following, i):
        @pl.when(i < tiles - 1)
        def _():
            in_copy(source, i + 1).start()
        if following is not None:
            @pl.when(i == tiles - 1)
            def _():
                in_copy(following, 0).start()
        in_copy(source, i).wait()
        return in_s[lax.rem(i, 2)]

    def at_tile(i):
        if isinstance(i, int):
            return pl.ds(i * TILE, TILE)
        return pl.ds(pl.multiple_of(i * TILE, TILE), TILE)

    def start(copies):
        for copy in copies:
            copy.start()

    def wait(copies):
        for copy in copies:
            copy.wait()

    def rows_of(a, slot):
        share = share_gu if a < 8 else share_d
        return pl.ds(pl.multiple_of(device(mask_of(PART[a], slot)) * share, 8), share)

    def own(layer, a, g, u, d):
        lo, hi = cols[a]
        return g.at[layer, :, lo:hi] if a < 4 else u.at[layer, :, lo - hidden:hi - hidden] if a < 8 else d.at[layer, :, lo:hi]

    def own_copy(layer, a):
        return pltpu.make_async_copy(own(layer, a, wg_hbm, wu_hbm, wd_hbm), slots[layer][a].at[0], own_sem.at[layer, a])

    def result_copy(layer, a):
        return pltpu.make_async_copy(slots[1][a].at[0], own(layer, a, og_hbm, ou_hbm, od_hbm), own_sem.at[layer, a])

    def gather_copy(layer, step, a):
        n = 2**step
        return pltpu.make_async_remote_copy(
            src_ref=slots[layer][a].at[pl.ds(0, n)], dst_ref=slots[layer][a].at[pl.ds(n, n)],
            send_sem=send_sem.at[layer, a, step], recv_sem=recv_sem.at[layer, a, step],
            device_id=to(PART[a] + STEPS - 1 - step), device_id_type=MESH)

    def hand_copy(layer, step, a):
        there = slots[layer][a].at[pl.ds(2**step, 2**step)]
        return pltpu.make_async_remote_copy(
            src_ref=there, dst_ref=there, send_sem=hand_send.at[layer, a, step], recv_sem=hand_recv.at[layer, a, step],
            device_id=partner, device_id_type=MESH)

    def by_core(arrays, act):
        for side in range(2):
            @pl.when(core == side)
            def _():
                act([a for a in arrays if keeper[a] == side], [a for a in arrays if keeper[a] != side])

    def gather_step(layer, step, arrays, then=None):
        def act(mine, _):
            for a in mine:
                if step > 0:
                    gather_copy(layer, step - 1, a).wait()
                if step < STEPS:
                    gather_copy(layer, step, a).start()
                if step > 0:
                    hand_copy(layer, step - 1, a).start()
        by_core(arrays, act)

    def gather_end(layer, arrays):
        def act(mine, others):
            for step in range(STEPS):
                for a in others:
                    hand_copy(layer, step, a).wait_recv()
                for a in mine:
                    hand_copy(layer, step, a).wait_send()
        by_core(arrays, act)

    def install(layer, arrays):
        for r in range(16):
            for a in arrays:
                lo, hi = cols[a]
                if a < 8:
                    wgu[layer, rows_of(a, r), lo:hi] = slots[layer][a][r]
                else:
                    acc_d[layer, rows_of(a, r), lo:hi] = slots[layer][a][r].astype(f32)

    def scatter_copy(layer, step, a):
        n = 2 ** (STEPS - 1 - step)
        return pltpu.make_async_remote_copy(
            src_ref=slots[1][a].at[pl.ds(n, n)], dst_ref=slots[0][a].at[pl.ds(n, n)],
            send_sem=send_sem.at[2 + layer, a, step], recv_sem=recv_sem.at[2 + layer, a, step],
            device_id=to(PART[a] + step), device_id_type=MESH)

    def scatter_start(layer, step, arrays):
        for a in arrays:
            if layer == 0:
                pl.semaphore_wait(credit.at[a, step], 1)
            scatter_copy(layer, step, a).start()

    def scatter_fill(layer, arrays):
        for a in arrays:
            lo, hi = cols[a]
            acc = acc_gu if a < 8 else acc_d
            for r in range(8, 16):
                slots[1][a][r] = acc[layer, rows_of(a, r), lo:hi].astype(bf16)
        scatter_start(layer, 0, arrays)

    def scatter_add(layer, step, arrays):
        n = 2 ** (STEPS - 1 - step)
        for a in arrays:
            lo, hi = cols[a]
            scatter_copy(layer, step, a).wait()
            acc = acc_gu if a < 8 else acc_d
            for r in reversed(range(n)):
                total = acc[layer, rows_of(a, r), lo:hi] + slots[0][a][n + r].astype(f32)
                if n == 1:
                    if layer == 0:
                        result_copy(1, a).wait()
                    slots[1][a][0] = total.astype(bf16)
                    result_copy(layer, a).start()
                elif r >= n // 2:
                    slots[1][a][r] = total.astype(bf16)
                else:
                    acc[layer, rows_of(a, r), lo:hi] = total
            if layer == 1:
                pl.semaphore_signal(credit.at[a, step], inc=1, device_id=to(PART[a] + step), device_id_type=MESH)
        if step < STEPS - 1:
            scatter_start(layer, step + 1, arrays)

    def chunks_of(lo, hi):
        return [(at, min(at + CHUNK, hi)) for at in range(lo, hi, CHUNK)]

    def normed(h):
        wide = h.astype(f32)
        scale = lax.rsqrt(jnp.mean(wide * wide, -1, keepdims=True) + 1e-6)
        return wide, scale, (wide * scale).astype(bf16)

    def loop(events, body, n=tiles):
        def step(i, _):
            for when, actions in events.items():
                @pl.when(i == when)
                def _():
                    for act, *args in actions:
                        act(*args)
            body(i)
            return 0
        lax.fori_loop(0, n, step, 0)

    def transposes(layer, down):
        for lo in range(0, 2 * hidden, CHUNK):
            wgut[lo:lo + CHUNK, :] = wgu[layer, :, lo:lo + CHUNK].T
        for lo, hi, block in down:
            wdt[:, lo:hi] = block[...].T.astype(bf16)

    def inner(g, u, dq):
        dq = dq.astype(bf16).astype(f32)
        sig = 0.5 * jnp.tanh(0.5 * g) + 0.5
        s = g * sig
        return (s * u).astype(bf16), (dq * u * (sig + s * (1 - sig))).astype(bf16), (dq * s).astype(bf16)

    def outer(wide, scale, dy, da):
        da = da.astype(bf16).astype(f32)
        mean = jnp.mean(da * wide, -1, keepdims=True)
        return dy + (da * scale - wide * (mean * scale * scale * scale)).astype(bf16)

    every = range(12)
    for layer in range(2):
        start([own_copy(layer, a) for a in every])
    in_copy(x_hbm, 0).start()
    barrier = pltpu.get_barrier_semaphore()
    for peer in [to(dim) for dim in range(4)] + [partner]:
        pl.semaphore_signal(barrier, inc=1, device_id=peer, device_id_type=MESH)
    wait([own_copy(0, a) for a in every])
    pl.semaphore_wait(barrier, 5)
    gather_step(0, 0, GU)
    gather_step(0, 0, D)
    gather_step(0, 1, GU)
    gather_step(0, 1, D)
    gather_step(0, 2, GU)
    gather_step(0, 2, D)
    gather_step(0, 3, GU)
    gather_step(0, 3, D)
    wait([own_copy(1, a) for a in every])
    gather_step(1, 0, every)
    in_copy(x_hbm, 0).wait()
    a_s[0] = normed(in_s[0])[2]
    gather_step(0, 4, GU)
    gather_end(0, GU)
    install(0, GU)

    def p_out(i):
        return pltpu.make_async_copy(p_s.at[lax.rem(i, 2)], p_hbm.at[at_tile(i)], p_sem.at[lax.rem(i, 2)])

    def gu_out(i):
        return pltpu.make_async_copy(acc_gu.at[lax.rem(i, 2)], gu_hbm.at[at_tile(i)], gu_sem.at[lax.rem(i, 2), 0])

    def a_out(i):
        return pltpu.make_async_copy(a_s.at[lax.rem(i, 2)], a_hbm.at[at_tile(i)], a_sem.at[lax.rem(i, 2)])

    def next_x(i):
        slot = lax.rem(i + 1, 2)
        return pltpu.make_async_copy(x_hbm.at[at_tile(jnp.minimum(i + 1, tiles - 1))], in_s.at[slot], in_sem.at[slot])

    def forward(i):
        slot = lax.rem(i, 2)
        next_x(i).start()
        a_out(i).start()

        @pl.when(i >= 1)
        def _():
            a_out(i - 1).wait()

        @pl.when(i >= 2)
        def _():
            p_out(i - 2).wait()
            gu_out(i - 2).wait()
        a = a_s[slot]
        for lo, hi in chunks_of(0, hidden):
            g, u = dot(a, wgu[0, :, lo:hi]), dot(a, wgu[0, :, hidden + lo:hidden + hi])
            acc_gu[slot, :, lo:hi] = g
            acc_gu[slot, :, hidden + lo:hidden + hi] = u
            p_s[slot, :, lo:hi] = (g * (0.5 * jnp.tanh(0.5 * g) + 0.5) * u).astype(bf16)
        p_out(i).start()
        gu_out(i).start()

        @pl.when(i == 0)
        def _():
            gather_step(0, 4, D)
            gather_end(0, D)
            install(0, D)
            for lo, hi, block in wd0:
                block[...] = acc_d[0, lo:hi].astype(bf16)
        next_x(i).wait()
        down = sum(dot(p_s[slot, :, lo:hi], block[...]) for lo, hi, block in wd0).astype(bf16)
        a_s[1 - slot] = normed(in_s[1 - slot])[2]
        h_s[at_tile(i), :] = in_s[slot] + down

    loop({1: [(gather_step, 1, 1, every)], 2: [(gather_step, 1, 2, every)], 4: [(gather_step, 1, 3, every)], 7: [(gather_step, 1, 4, every)]}, forward)
    a_out(tiles - 1).wait()
    in_copy(dy_hbm, 0).start()
    gather_end(1, every)
    install(1, every)
    transposes(1, [(lo, hi, acc_d.at[1, lo:hi]) for lo, hi in chunks_of(0, hidden)])
    acc_d[...] = jnp.zeros_like(acc_d)
    for i in (tiles - 2, tiles - 1):
        p_out(i).wait()
        gu_out(i).wait()
    acc_gu[...] = jnp.zeros_like(acc_gu)

    def p_in(i):
        return pltpu.make_async_copy(p_hbm.at[at_tile(i)], p_s.at[1], p_sem.at[0])

    def last(i):
        rows = at_tile(i)
        wide, scale, a = normed(h_s[rows, :])
        dy = streamed(dy_hbm, a_hbm, i)
        for lo, hi in chunks_of(0, hidden):
            g, u = dot(a, wgu[1, :, lo:hi]), dot(a, wgu[1, :, hidden + lo:hidden + hi])
            p_s[0, :, lo:hi], dgu_s[0, :, lo:hi], dgu_s[0, :, hidden + lo:hidden + hi] = inner(g, u, dot(dy, wdt[:, lo:hi]))
        dh = outer(wide, scale, dy, dot(dgu_s[0], wgut[...]))
        h_s[rows, :] = dh
        acc_d[1] += dot_t(p_s[0], dy)
        acc_gu[1] += dot_t(a, dgu_s[0])
        p_in(i).wait()
        acc_d[0] += dot_t(p_s[1], dh)

        @pl.when(i < tiles - 1)
        def _():
            p_in(i + 1).start()

    p_in(0).start()
    loop({}, last)
    scatter_fill(1, every)
    transposes(0, [(lo, min(lo + CHUNK, hi), block.at[lo - begin:min(lo + CHUNK, hi) - begin]) for begin, hi, block in wd0 for lo in range(begin, hi, CHUNK)])

    def dgu_copies(i, span, out):
        slot = lax.rem(i, 2)
        found = []
        for side in range(2):
            place = pl.ds(side * hidden + span[0], span[1] - span[0])
            there, here = dgu_hbm.at[at_tile(i), place], dgu_s.at[slot, :, place]
            found.append(pltpu.make_async_copy(*((here, there) if out else (there, here)), dgu_sem.at[slot, side]))
        return found

    def gu_in(i, span):
        slot, n = lax.rem(i, 2), span[1] - span[0]
        return [pltpu.make_async_copy(gu_hbm.at[at_tile(i), pl.ds(side * hidden + span[0], n)], gu_s.at[slot, :, pl.ds(side * half, n)],
                                      gu_sem.at[slot, side]) for side in range(2)]

    def gate_up(i, span, following):
        slot = lax.rem(i, 2)
        dy = h_s[at_tile(i), :]
        a = streamed(a_hbm, following, i)

        @pl.when(i < tiles - 1)
        def _():
            start(gu_in(i + 1, span))

        @pl.when(i >= 2)
        def _():
            wait(dgu_copies(i - 2, span, True))
        wait(gu_in(i, span))
        for lo, hi in chunks_of(*span):
            here = [slice(at + lo - span[0], at + hi - span[0]) for at in (0, half)]
            _, dgu_s[slot, :, lo:hi], dgu_s[slot, :, hidden + lo:hidden + hi] = inner(gu_s[slot, :, here[0]], gu_s[slot, :, here[1]], dot(dy, wdt[:, lo:hi]))
        start(dgu_copies(i, span, True))
        for side in range(2):
            lo, hi = (side * hidden + at for at in span)
            acc_gu[0, :, lo:hi] += dot_t(a, dgu_s[slot, :, lo:hi])

    def drain(span):
        for i in range(tiles - 2, tiles):
            wait(dgu_copies(i, span, True))

    whole, da_s = (0, hidden), gu_s.at[0, :, :width]

    def back(i, last=False):
        rows = at_tile(i)
        if not last:
            @pl.when(i < tiles - 2)
            def _():
                start(dgu_copies(i + 2, whole, False))
            wait(dgu_copies(i + 1, whole, False))
            x = streamed(x_hbm, None, i)
        else:
            in_copy(x_hbm, i).wait()
            x = in_s[i % 2]
        wide, scale, _ = normed(x)
        h_s[rows, :] = outer(wide, scale, h_s[rows, :], da_s[...])
        if not last:
            da_s[...] = dot(dgu_s[lax.rem(i + 1, 2)], wgut[...])

    first, second = (0, half), (half, hidden)
    start(gu_in(0, first))
    loop({7: [(scatter_add, 1, 0, every)]}, lambda i: gate_up(i, first, a_hbm))
    start(gu_in(0, second))
    scatter_fill(0, D)
    drain(first)
    scatter_fill(0, FIRST)
    loop({4: [(scatter_add, 1, 1, every)], 6: [(scatter_add, 0, 0, D), (scatter_add, 0, 0, FIRST)]}, lambda i: gate_up(i, second, x_hbm))
    drain(second)
    for i in range(2):
        start(dgu_copies(i, whole, False))
    scatter_fill(0, SECOND)
    scatter_add(1, 2, every)
    wait(dgu_copies(0, whole, False))
    da_s[...] = dot(dgu_s[0], wgut[...])
    loop({0: [(scatter_add, 0, 1, D), (scatter_add, 0, 1, FIRST)],
          2: [(scatter_add, 1, 3, every), (scatter_add, 0, 0, SECOND)], 3: [(scatter_add, 0, 2, D), (scatter_add, 0, 2, FIRST)],
          4: [(scatter_add, 0, 1, SECOND)], 5: [(scatter_add, 0, 3, D), (scatter_add, 0, 3, FIRST)], 6: [(scatter_add, 0, 2, SECOND)]}, back, tiles - 1)
    back(tiles - 1, True)
    scatter_add(0, 3, SECOND)
    wait([result_copy(0, a) for a in every])


def pieces_of(hidden):
    lanes = hidden // 128
    cuts = [128 * -(-lanes * q // 4) for q in range(5)]
    return list(zip(cuts, cuts[1:]))


def solution(mesh):
    group = mesh.shape["dp"]
    side = math.isqrt(group)
    assert side * side == group == 2**STEPS

    def local(x, dy, w_gate, w_up, w_down):
        _, tokens, width = x.shape
        layers, share_gu, hidden = w_gate.shape
        share_d = w_down.shape[1]
        parts = [pltpu.VMEM((group, share_gu, hi - lo), bf16) for lo, hi in pieces_of(hidden) * 2]
        parts += [pltpu.VMEM((group, share_d, width // 4), bf16)] * 4
        any_, vmem = pl.BlockSpec(memory_space=pl.ANY), pl.BlockSpec(memory_space=pltpu.VMEM)
        shapes = ((tokens, width), w_gate.shape, w_up.shape, w_down.shape, (tokens, hidden), (tokens, 2 * hidden), (tokens, width))
        dma = pltpu.SemaphoreType.DMA
        out = pl.pallas_call(
            functools.partial(kernel, (tokens, width, hidden, share_gu, share_d)),
            out_shape=[jax.ShapeDtypeStruct(s, bf16) for s in shapes] + [jax.ShapeDtypeStruct((tokens, 2 * hidden), f32)],
            in_specs=[any_] * 5,
            out_specs=[vmem] + [any_] * 7,
            scratch_shapes=[
                pltpu.VMEM((2, TILE, width), bf16),
                pltpu.VMEM((2, TILE, 2 * pieces_of(hidden)[2][0]), f32),
                pltpu.VMEM((layers, width, 2 * hidden), bf16),
                pltpu.VMEM((2 * hidden, width), bf16),
                pltpu.VMEM((width, hidden), bf16),
                pltpu.VMEM((layers, width, 2 * hidden), f32),
                pltpu.VMEM((layers, hidden, width), f32),
                pltpu.VMEM((2, TILE, hidden), bf16),
                pltpu.VMEM((2, TILE, 2 * hidden), bf16),
            ] + parts * 2 + [
                dma((4, 12, STEPS)), dma((4, 12, STEPS)), dma((2, 12, STEPS)), dma((2, 12, STEPS)),
                pltpu.SemaphoreType.REGULAR((12, STEPS)), dma((2, 12)), dma((2,)), dma((2,)), dma((2,)), dma((2, 2)), dma((2, 2)),
            ],
            compiler_params=pltpu.CompilerParams(collective_id=0, has_side_effects=True, vmem_limit_bytes=VMEM_LIMIT),
            name="stack",
        )(x[0], dy[0], w_gate, w_up, w_down)
        return (out[0][None], *out[1:4])

    tokens_spec = P(("rep", "dp"), None, None)
    weight_spec, grad_spec = P(None, "dp", None), P("rep", "dp", None)
    return jax.shard_map(local, mesh=mesh, in_specs=(tokens_spec, tokens_spec) + (weight_spec,) * 3,
                         out_specs=(tokens_spec,) + (grad_spec,) * 3, check_vma=False)
```

```python
import functools
import math

import jax
import jax.numpy as jnp
from jax import lax
from jax.experimental import pallas as pl
from jax.experimental.pallas import tpu as pltpu
from jax.sharding import PartitionSpec as P

bf16, f32 = jnp.bfloat16, jnp.float32
MESH = pl.DeviceIdType.MESH
TILE = 512
CHUNK = 256
STEPS = 4
GATHER = (((0, 1, 1, 1), (0, 2, 1, 2), (0, 3, 1, 3)), ((0, 4, 4, 4),), ((0, 8, 8, 8),))
SCATTER = (((8, 8, 8, 8),), ((4, 4, 4, 4),), ((1, 1, 1, 1), (2, 2, 1, 2), (3, 3, 1, 3)))
ROUNDS = 3
VMEM_LIMIT = 67043328
DIMS = ((1, 0), (0, 1), (3, 0), (0, 3))
PART = (0, 1, 0, 1, 2, 3, 2, 3, 0, 1, 2, 3)


def dot(a, b):
    return jnp.dot(a, b, preferred_element_type=f32)


def dot_t(a, b):
    return lax.dot_general(a, b, (((0,), (0,)), ((), ())), preferred_element_type=f32)


def flip(c, bits):
    return (c, c + 1 - 2 * lax.rem(c, 2), lax.rem(c + 2, 4), 3 - c)[bits]


def mask_of(part, slot):
    x = y = 0
    for bit in range(STEPS):
        if slot >> bit & 1:
            dx, dy = DIMS[(part + STEPS - 1 - bit) % 4]
            x, y = x ^ dx, y ^ dy
    return x, y


def kernel(sizes, x_hbm, dy_hbm, wg_hbm, wu_hbm, wd_hbm, dx_hbm, og_hbm, ou_hbm, od_hbm, p_hbm, dgu_hbm, a_hbm, gu_hbm, *scratch):
    (in_s, h_s, gu_s, wgu, wgut, wdt, acc_gu, acc_d, p_s, dgu_s, *rest) = scratch
    slots = (rest[:12], rest[12:24])
    send_sem, recv_sem, hand_send, hand_recv, credit, own_sem, in_sem, a_sem, p_sem, dgu_sem, gu_sem, dx_sem, ready = rest[24:]
    tokens, width, hidden, share_gu, share_d = sizes
    a_s = dgu_s.at[:, :, :width]
    wd0 = [(lo, min(lo + TILE, hidden), dgu_s.at[1, :min(TILE, hidden - lo), pl.ds((1 + lo // TILE) * width, width)]) for lo in range(0, hidden, TILE)]
    me, rep = lax.axis_index("dp"), lax.axis_index("rep")
    mx, my = lax.div(me, 4), lax.rem(me, 4)
    core = lax.rem(rep, 2)
    tiles = tokens // TILE

    def device(mask):
        return flip(mx, mask[0]) * 4 + flip(my, mask[1])

    def to(a, slot):
        return {"dp": device(mask_of(PART[a], slot))}

    partner = {"rep": rep + 1 - 2 * core}
    pieces = pieces_of(hidden)
    cols = pieces + [(hidden + lo, hidden + hi) for lo, hi in pieces] + [(width * q // 4, width * (q + 1) // 4) for q in range(4)]
    GU, D = range(8), range(8, 12)
    half = pieces[2][0]
    FIRST, SECOND = (0, 1, 4, 5), (2, 3, 6, 7)
    keeper = (0, 0, 0, 0, 1, 1, 1, 1, 0, 0, 1, 1)

    def in_copy(source, i):
        return pltpu.make_async_copy(source.at[at_tile(i)], in_s.at[lax.rem(i, 2)], in_sem.at[lax.rem(i, 2)])

    def streamed(source, following, i):
        @pl.when(i < tiles - 1)
        def _():
            in_copy(source, i + 1).start()
        if following is not None:
            @pl.when(i == tiles - 1)
            def _():
                in_copy(following, 0).start()
        in_copy(source, i).wait()
        return in_s[lax.rem(i, 2)]

    def at_tile(i):
        if isinstance(i, int):
            return pl.ds(i * TILE, TILE)
        return pl.ds(pl.multiple_of(i * TILE, TILE), TILE)

    def start(copies):
        for copy in copies:
            copy.start()

    def wait(copies):
        for copy in copies:
            copy.wait()

    def rows_of(a, slot):
        share = share_gu if a < 8 else share_d
        return pl.ds(pl.multiple_of(device(mask_of(PART[a], slot)) * share, 8), share)

    def own(layer, a, g, u, d):
        lo, hi = cols[a]
        return g.at[layer, :, lo:hi] if a < 4 else u.at[layer, :, lo - hidden:hi - hidden] if a < 8 else d.at[layer, :, lo:hi]

    def own_copy(layer, a):
        return pltpu.make_async_copy(own(layer, a, wg_hbm, wu_hbm, wd_hbm), slots[layer][a].at[0], own_sem.at[layer, a])

    def result_copy(layer, a):
        return pltpu.make_async_copy(slots[1][a].at[0], own(layer, a, og_hbm, ou_hbm, od_hbm), own_sem.at[layer, a])

    def exchange(kind, a, rounds, n, source, target):
        before = sum(len(r) for r in rounds[:n])
        return [pltpu.make_async_remote_copy(
            src_ref=source[a].at[pl.ds(here, count)], dst_ref=target[a].at[pl.ds(there, count)],
            send_sem=send_sem.at[kind, a, before + k], recv_sem=recv_sem.at[kind, a, before + k],
            device_id=to(a, slot), device_id_type=MESH) for k, (here, there, count, slot) in enumerate(rounds[n])]

    def gather_copies(layer, n, a):
        return exchange(layer, a, GATHER, n, slots[layer], slots[layer])

    def hand_copy(layer, n, a):
        there = slots[layer][a].at[pl.ds(*((1, 3), (4, 4), (8, 8))[n])]
        return pltpu.make_async_remote_copy(
            src_ref=there, dst_ref=there, send_sem=hand_send.at[layer, a, n], recv_sem=hand_recv.at[layer, a, n],
            device_id=partner, device_id_type=MESH)

    def by_core(arrays, act):
        for side in range(2):
            @pl.when(core == side)
            def _():
                act([a for a in arrays if keeper[a] == side], [a for a in arrays if keeper[a] != side])

    def gather_step(layer, n, arrays):
        def act(mine, _):
            for a in mine:
                if n > 0:
                    wait(gather_copies(layer, n - 1, a))
                if n < ROUNDS:
                    start(gather_copies(layer, n, a))
                if n > 0:
                    hand_copy(layer, n - 1, a).start()
        by_core(arrays, act)

    def gather_end(layer, arrays):
        def act(mine, others):
            for n in range(ROUNDS):
                for a in others:
                    hand_copy(layer, n, a).wait_recv()
                for a in mine:
                    hand_copy(layer, n, a).wait_send()
        by_core(arrays, act)

    def install(layer, arrays):
        for r in range(16):
            for a in arrays:
                lo, hi = cols[a]
                if a < 8:
                    wgu[layer, rows_of(a, r), lo:hi] = slots[layer][a][r]
                else:
                    acc_d[layer, rows_of(a, r), lo:hi] = slots[layer][a][r].astype(f32)

    def scatter_copies(layer, n, a):
        return exchange(2 + layer, a, SCATTER, n, slots[1], slots[0])

    def scatter_start(layer, n, arrays):
        for a in arrays:
            before = sum(len(r) for r in SCATTER[:n])
            for k, copy in enumerate(scatter_copies(layer, n, a)):
                if layer == 0:
                    pl.semaphore_wait(credit.at[a, before + k], 1)
                copy.start()

    def scatter_fill(layer, arrays):
        for a in arrays:
            lo, hi = cols[a]
            acc = acc_gu if a < 8 else acc_d
            for r in range(8, 16):
                slots[1][a][r] = acc[layer, rows_of(a, r), lo:hi].astype(bf16)
        scatter_start(layer, 0, arrays)

    def scatter_add(layer, n, arrays):
        keep, stay = ((8, 4), (4, 1), (1, 0))[n]
        for a in arrays:
            lo, hi = cols[a]
            acc = acc_gu if a < 8 else acc_d
            wait(scatter_copies(layer, n, a))
            for r in reversed(range(keep)):
                total = acc[layer, rows_of(a, r), lo:hi]
                for _, there, count, _ in SCATTER[n]:
                    if r < count:
                        total += slots[0][a][there + r].astype(f32)
                if n == ROUNDS - 1:
                    if layer == 0:
                        result_copy(1, a).wait()
                    slots[1][a][0] = total.astype(bf16)
                    result_copy(layer, a).start()
                elif r >= stay:
                    slots[1][a][r] = total.astype(bf16)
                else:
                    acc[layer, rows_of(a, r), lo:hi] = total
            if layer == 1:
                before = sum(len(r) for r in SCATTER[:n])
                for k, (_, _, _, slot) in enumerate(SCATTER[n]):
                    pl.semaphore_signal(credit.at[a, before + k], inc=1, device_id=to(a, slot), device_id_type=MESH)
        if n < ROUNDS - 1:
            scatter_start(layer, n + 1, arrays)

    def chunks_of(lo, hi):
        return [(at, min(at + CHUNK, hi)) for at in range(lo, hi, CHUNK)]

    def normed(h):
        wide = h.astype(f32)
        scale = lax.rsqrt(jnp.mean(wide * wide, -1, keepdims=True) + 1e-6)
        return wide, scale, (wide * scale).astype(bf16)

    def loop(events, body, n=tiles):
        def step(i, _):
            for when, actions in events.items():
                @pl.when(i == when)
                def _():
                    for act, *args in actions:
                        act(*args)
            body(i)
            return 0
        lax.fori_loop(0, n, step, 0)

    def transposes(layer, down):
        for lo in range(0, 2 * hidden, CHUNK):
            wgut[lo:lo + CHUNK, :] = wgu[layer, :, lo:lo + CHUNK].T
        for lo, hi, block in down:
            wdt[:, lo:hi] = block[...].T.astype(bf16)

    def inner(g, u, dq):
        dq = dq.astype(bf16).astype(f32)
        sig = 0.5 * jnp.tanh(0.5 * g) + 0.5
        s = g * sig
        return (s * u).astype(bf16), (dq * u * (sig + s * (1 - sig))).astype(bf16), (dq * s).astype(bf16)

    def outer(wide, scale, dy, da):
        da = da.astype(bf16).astype(f32)
        mean = jnp.mean(da * wide, -1, keepdims=True)
        return dy + (da * scale - wide * (mean * scale * scale * scale)).astype(bf16)

    every = range(12)
    for layer in range(2):
        start([own_copy(layer, a) for a in every])
    in_copy(x_hbm, 0).start()
    barrier = pltpu.get_barrier_semaphore()
    peers = [to(a, slot) for a in range(8, 12) for slot in (1, 3)]
    for peer in peers + [partner]:
        pl.semaphore_signal(barrier, inc=1, device_id=peer, device_id_type=MESH)
    wait([own_copy(0, a) for a in every])
    pl.semaphore_wait(barrier, 9)
    for n in range(ROUNDS):
        gather_step(0, n, GU)
        gather_step(0, n, D)
    wait([own_copy(1, a) for a in every])
    gather_step(1, 0, every)
    in_copy(x_hbm, 0).wait()
    a_s[0] = normed(in_s[0])[2]
    gather_step(0, ROUNDS, GU)
    gather_end(0, GU)
    install(0, GU)

    def p_out(i):
        return pltpu.make_async_copy(p_s.at[lax.rem(i, 2)], p_hbm.at[at_tile(i)], p_sem.at[lax.rem(i, 2)])

    def gu_out(i):
        return pltpu.make_async_copy(acc_gu.at[lax.rem(i, 2)], gu_hbm.at[at_tile(i)], gu_sem.at[lax.rem(i, 2), 0])

    def a_out(i):
        return pltpu.make_async_copy(a_s.at[lax.rem(i, 2)], a_hbm.at[at_tile(i)], a_sem.at[lax.rem(i, 2)])

    def next_x(i):
        slot = lax.rem(i + 1, 2)
        return pltpu.make_async_copy(x_hbm.at[at_tile(jnp.minimum(i + 1, tiles - 1))], in_s.at[slot], in_sem.at[slot])

    def down(slot):
        return sum(dot(p_s[slot, :, lo:hi], block[...]) for lo, hi, block in wd0).astype(bf16)

    def forward(i):
        slot = lax.rem(i, 2)
        next_x(i).start()
        a_out(i).start()

        @pl.when(i >= 1)
        def _():
            a_out(i - 1).wait()

        @pl.when(i >= 2)
        def _():
            p_out(i - 2).wait()
            gu_out(i - 2).wait()

        @pl.when(i == 1)
        def _():
            gather_step(0, ROUNDS, D)
            gather_end(0, D)
            install(0, D)
            for lo, hi, block in wd0:
                block[...] = acc_d[0, lo:hi].astype(bf16)
            for peer in peers:
                pl.semaphore_signal(ready, inc=1, device_id=peer, device_id_type=MESH)
        before = at_tile(jnp.maximum(i - 1, 0))
        h_s[before, :] += down(1 - slot)
        h_s[at_tile(i), :] = in_s[slot]
        a = a_s[slot]
        for lo, hi in chunks_of(0, hidden):
            g, u = dot(a, wgu[0, :, lo:hi]), dot(a, wgu[0, :, hidden + lo:hidden + hi])
            acc_gu[slot, :, lo:hi] = g
            acc_gu[slot, :, hidden + lo:hidden + hi] = u
            p_s[slot, :, lo:hi] = (g * (0.5 * jnp.tanh(0.5 * g) + 0.5) * u).astype(bf16)
        p_out(i).start()
        gu_out(i).start()
        next_x(i).wait()
        a_s[1 - slot] = normed(in_s[1 - slot])[2]

    loop({1: [(gather_step, 1, 1, every)], 3: [(gather_step, 1, 2, every)], 7: [(gather_step, 1, ROUNDS, every)]}, forward)
    h_s[at_tile(tiles - 1), :] += down((tiles - 1) % 2)
    a_out(tiles - 1).wait()
    in_copy(dy_hbm, 0).start()
    gather_end(1, every)
    install(1, every)
    transposes(1, [(lo, hi, acc_d.at[1, lo:hi]) for lo, hi in chunks_of(0, hidden)])
    acc_d[...] = jnp.zeros_like(acc_d)
    for i in (tiles - 2, tiles - 1):
        p_out(i).wait()
        gu_out(i).wait()
    acc_gu[...] = jnp.zeros_like(acc_gu)

    first, second = (0, half), (half, hidden)

    def gu_in(i, span):
        slot, n = lax.rem(i, 2), span[1] - span[0]
        return [pltpu.make_async_copy(gu_hbm.at[at_tile(i), pl.ds(side * hidden + span[0], n)], gu_s.at[slot, :, pl.ds(side * half, n)],
                                      gu_sem.at[slot, side]) for side in range(2)]

    def p_in(i):
        return pltpu.make_async_copy(p_hbm.at[at_tile(i)], p_s.at[lax.rem(i, 2)], p_sem.at[lax.rem(i, 2)])

    def last(i):
        rows = at_tile(i)
        wide, scale, a = normed(h_s[rows, :])
        dy = streamed(dy_hbm, a_hbm, i)
        for lo, hi in chunks_of(0, hidden):
            g, u = dot(a, wgu[1, :, lo:hi]), dot(a, wgu[1, :, hidden + lo:hidden + hi])
            p_s[0, :, lo:hi], dgu_s[0, :, lo:hi], dgu_s[0, :, hidden + lo:hidden + hi] = inner(g, u, dot(dy, wdt[:, lo:hi]))
        h_s[rows, :] = outer(wide, scale, dy, dot(dgu_s[0], wgut[...]))
        acc_d[1] += dot_t(p_s[0], dy)
        acc_gu[1] += dot_t(a, dgu_s[0])

    start(gu_in(0, first))
    loop({}, last)
    p_in(0).start()
    pl.semaphore_wait(ready, len(peers))
    for arrays in (FIRST, SECOND, D):
        scatter_fill(1, arrays)
    transposes(0, [(lo, min(lo + CHUNK, hi), block.at[lo - begin:min(lo + CHUNK, hi) - begin]) for begin, hi, block in wd0 for lo in range(begin, hi, CHUNK)])

    def dgu_copies(i, span, out):
        slot = lax.rem(i, 2)
        found = []
        for side in range(2):
            place = pl.ds(side * hidden + span[0], span[1] - span[0])
            there, here = dgu_hbm.at[at_tile(i), place], dgu_s.at[slot, :, place]
            found.append(pltpu.make_async_copy(*((here, there) if out else (there, here)), dgu_sem.at[slot, side, int(out)]))
        return found

    def gate_up(i, span, following, after, down=False):
        slot = lax.rem(i, 2)
        dy = h_s[at_tile(i), :]
        a = streamed(a_hbm, following, i)
        if down:
            @pl.when(i < tiles - 1)
            def _():
                p_in(i + 1).start()
            p_in(i).wait()

        @pl.when(i < tiles - 1)
        def _():
            start(gu_in(i + 1, span))

        @pl.when(i == tiles - 1)
        def _():
            after()

        @pl.when(i >= 2)
        def _():
            wait(dgu_copies(i - 2, span, True))
        wait(gu_in(i, span))
        if down:
            acc_d[0] += dot_t(p_s[slot], dy)
        for lo, hi in chunks_of(*span):
            here = [slice(at + lo - span[0], at + hi - span[0]) for at in (0, half)]
            _, dgu_s[slot, :, lo:hi], dgu_s[slot, :, hidden + lo:hidden + hi] = inner(gu_s[slot, :, here[0]], gu_s[slot, :, here[1]], dot(dy, wdt[:, lo:hi]))
        for side in range(2):
            lo, hi = (side * hidden + at for at in span)
            acc_gu[0, :, lo:hi] += dot_t(a, dgu_s[slot, :, lo:hi])
        start(dgu_copies(i, span, True))

    def drain(span):
        for i in range(tiles - 2, tiles):
            wait(dgu_copies(i, span, True))

    whole, da_s = (0, hidden), gu_s.at[0, :, :width]

    def x_in(i):
        tile = tiles - 1 - i
        return pltpu.make_async_copy(x_hbm.at[at_tile(tile)], in_s.at[lax.rem(i, 2)], in_sem.at[lax.rem(i, 2)])

    def dgu_in(i):
        return dgu_copies(tiles - 1 - i, whole, False)

    def dx_out(i):
        rows = at_tile(tiles - 1 - i)
        return pltpu.make_async_copy(h_s.at[rows], dx_hbm.at[rows], dx_sem.at[i])

    def back(i):
        rows = at_tile(tiles - 1 - i)
        if isinstance(i, int):
            x_in(i).wait()
            ahead = i < tiles - 1
        else:
            @pl.when(i < tiles - 2)
            def _():
                start(dgu_in(i + 2))

            @pl.when(i >= 1)
            def _():
                wait(dgu_in(i + 1))
            x_in(i + 1).start()
            x_in(i).wait()
            ahead = True
        wide, scale, _ = normed(in_s[i % 2 if isinstance(i, int) else lax.rem(i, 2)])
        h_s[rows, :] = outer(wide, scale, h_s[rows, :], da_s[...])
        dx_out(i).start()
        if ahead:
            da_s[...] = dot(dgu_s[lax.rem(tiles - 2 - i, 2)], wgut[...])

    loop({3: [(scatter_add, 1, 0, FIRST)], 4: [(scatter_add, 1, 0, SECOND)], 6: [(scatter_add, 1, 0, D), (scatter_add, 1, 1, FIRST)],
          7: [(scatter_add, 1, 1, SECOND)]}, lambda i: gate_up(i, first, a_hbm, lambda: start(gu_in(0, second)), True))
    scatter_add(1, 1, D)
    scatter_fill(0, D)
    drain(first)
    scatter_fill(0, FIRST)
    loop({1: [(scatter_add, 1, 2, FIRST)], 2: [(scatter_add, 1, 2, SECOND)], 3: [(scatter_add, 1, 2, D)], 5: [(scatter_add, 0, 0, D)],
          7: [(scatter_add, 0, 0, FIRST)]}, lambda i: gate_up(i, second, None, lambda: x_in(0).start()))
    drain(second)
    scatter_add(0, 1, D)
    scatter_fill(0, SECOND)
    da_s[...] = dot(dgu_s[(tiles - 1) % 2], wgut[...])
    loop({1: [(scatter_add, 0, 1, FIRST)], 2: [(scatter_add, 0, 2, D)], 3: [(scatter_add, 0, 0, SECOND)], 5: [(scatter_add, 0, 2, FIRST)],
          6: [(scatter_add, 0, 1, SECOND)]}, back, tiles - 1)
    back(tiles - 1)
    scatter_add(0, 2, SECOND)
    wait([dx_out(i) for i in range(tiles)])
    wait([result_copy(0, a) for a in every])


def pieces_of(hidden):
    lanes = hidden // 128
    cuts = [128 * -(-lanes * q // 4) for q in range(5)]
    return list(zip(cuts, cuts[1:]))


def solution(mesh):
    group = mesh.shape["dp"]
    side = math.isqrt(group)
    assert side * side == group == 2**STEPS

    def local(x, dy, w_gate, w_up, w_down):
        _, tokens, width = x.shape
        layers, share_gu, hidden = w_gate.shape
        share_d = w_down.shape[1]
        parts = [pltpu.VMEM((group, share_gu, hi - lo), bf16) for lo, hi in pieces_of(hidden) * 2]
        parts += [pltpu.VMEM((group, share_d, width // 4), bf16)] * 4
        any_, vmem = pl.BlockSpec(memory_space=pl.ANY), pl.BlockSpec(memory_space=pltpu.VMEM)
        shapes = ((tokens, width), w_gate.shape, w_up.shape, w_down.shape, (tokens, hidden), (tokens, 2 * hidden), (tokens, width))
        dma = pltpu.SemaphoreType.DMA
        out = pl.pallas_call(
            functools.partial(kernel, (tokens, width, hidden, share_gu, share_d)),
            out_shape=[jax.ShapeDtypeStruct(s, bf16) for s in shapes] + [jax.ShapeDtypeStruct((tokens, 2 * hidden), f32)],
            in_specs=[any_] * 5,
            out_specs=[any_] * 8,
            scratch_shapes=[
                pltpu.VMEM((2, TILE, width), bf16),
                pltpu.VMEM((tokens, width), bf16),
                pltpu.VMEM((2, TILE, 2 * pieces_of(hidden)[2][0]), f32),
                pltpu.VMEM((layers, width, 2 * hidden), bf16),
                pltpu.VMEM((2 * hidden, width), bf16),
                pltpu.VMEM((width, hidden), bf16),
                pltpu.VMEM((layers, width, 2 * hidden), f32),
                pltpu.VMEM((layers, hidden, width), f32),
                pltpu.VMEM((2, TILE, hidden), bf16),
                pltpu.VMEM((2, TILE, 2 * hidden), bf16),
            ] + parts * 2 + [
                dma((4, 12, 5)), dma((4, 12, 5)), dma((2, 12, ROUNDS)), dma((2, 12, ROUNDS)),
                pltpu.SemaphoreType.REGULAR((12, 5)), dma((2, 12)), dma((2,)), dma((2,)), dma((2,)), dma((2, 2, 2)), dma((2, 2)), dma((tokens // TILE,)),
                pltpu.SemaphoreType.REGULAR,
            ],
            compiler_params=pltpu.CompilerParams(collective_id=0, has_side_effects=True, vmem_limit_bytes=VMEM_LIMIT),
            name="stack",
        )(x[0], dy[0], w_gate, w_up, w_down)
        return (out[0][None], *out[1:4])

    tokens_spec = P(("rep", "dp"), None, None)
    weight_spec, grad_spec = P(None, "dp", None), P("rep", "dp", None)
    return jax.shard_map(local, mesh=mesh, in_specs=(tokens_spec, tokens_spec) + (weight_spec,) * 3,
                         out_specs=(tokens_spec,) + (grad_spec,) * 3, check_vma=False)
```

```python
import functools
import math

import jax
import jax.numpy as jnp
from jax import lax
from jax.experimental import pallas as pl
from jax.experimental.pallas import tpu as pltpu
from jax.sharding import PartitionSpec as P

bf16, f32 = jnp.bfloat16, jnp.float32
MESH = pl.DeviceIdType.MESH
TILE = 512
CHUNK = 256
STEPS = 4
GATHER = (((0, 1, 1, 1), (0, 2, 1, 2), (0, 3, 1, 3)), ((0, 4, 4, 4),), ((0, 8, 8, 8),))
SCATTER = (((8, 8, 8, 8),), ((4, 4, 4, 4),), ((1, 1, 1, 1), (2, 2, 1, 2), (3, 3, 1, 3)))
ROUNDS = 3
VMEM_LIMIT = 67043328
DIMS = ((1, 0), (0, 1), (3, 0), (0, 3))
PART = (0, 1, 0, 1, 2, 3, 2, 3, 0, 1, 2, 3)


def dot(a, b):
    return jnp.dot(a, b, preferred_element_type=f32)


def dot_t(a, b):
    return lax.dot_general(a, b, (((0,), (0,)), ((), ())), preferred_element_type=f32)


def flip(c, bits):
    return (c, c + 1 - 2 * lax.rem(c, 2), lax.rem(c + 2, 4), 3 - c)[bits]


def mask_of(part, slot):
    x = y = 0
    for bit in range(STEPS):
        if slot >> bit & 1:
            dx, dy = DIMS[(part + STEPS - 1 - bit) % 4]
            x, y = x ^ dx, y ^ dy
    return x, y


def kernel(sizes, x_hbm, dy_hbm, wg_hbm, wu_hbm, wd_hbm, dx_hbm, og_hbm, ou_hbm, od_hbm, p_hbm, dgu_hbm, a_hbm, gu_hbm, *scratch):
    (in_s, h_s, gu_s, wgu, wgut, wdt, acc_gu, acc_d, p_s, dgu_s, *rest) = scratch
    slots = (rest[:12], rest[12:24])
    send_sem, recv_sem, hand_send, hand_recv, credit, own_sem, in_sem, a_sem, p_sem, dgu_sem, gu_sem, dx_sem, ready = rest[24:]
    tokens, width, hidden, share_gu, share_d = sizes
    a_s = dgu_s.at[:, :, :width]
    wd0 = [(lo, min(lo + TILE, hidden), dgu_s.at[1, :min(TILE, hidden - lo), pl.ds((1 + lo // TILE) * width, width)]) for lo in range(0, hidden, TILE)]
    me, rep = lax.axis_index("dp"), lax.axis_index("rep")
    mx, my = lax.div(me, 4), lax.rem(me, 4)
    core = lax.rem(rep, 2)
    tiles = tokens // TILE

    def device(mask):
        return flip(mx, mask[0]) * 4 + flip(my, mask[1])

    def to(a, slot):
        return {"dp": device(mask_of(PART[a], slot))}

    partner = {"rep": rep + 1 - 2 * core}
    pieces = pieces_of(hidden)
    cols = pieces + [(hidden + lo, hidden + hi) for lo, hi in pieces] + [(width * q // 4, width * (q + 1) // 4) for q in range(4)]
    GU, D = range(8), range(8, 12)
    half = pieces[2][0]
    FIRST, SECOND = (0, 1, 4, 5), (2, 3, 6, 7)
    keeper = (0, 0, 0, 0, 1, 1, 1, 1, 0, 0, 1, 1)

    def in_copy(source, i):
        return pltpu.make_async_copy(source.at[at_tile(i)], in_s.at[lax.rem(i, 2)], in_sem.at[lax.rem(i, 2)])

    def streamed(source, following, i):
        @pl.when(i < tiles - 1)
        def _():
            in_copy(source, i + 1).start()
        if following is not None:
            @pl.when(i == tiles - 1)
            def _():
                in_copy(following, 0).start()
        in_copy(source, i).wait()
        return in_s[lax.rem(i, 2)]

    def at_tile(i):
        if isinstance(i, int):
            return pl.ds(i * TILE, TILE)
        return pl.ds(pl.multiple_of(i * TILE, TILE), TILE)

    def start(copies):
        for copy in copies:
            copy.start()

    def wait(copies):
        for copy in copies:
            copy.wait()

    def rows_of(a, slot):
        share = share_gu if a < 8 else share_d
        return pl.ds(pl.multiple_of(device(mask_of(PART[a], slot)) * share, 8), share)

    def own(layer, a, g, u, d):
        lo, hi = cols[a]
        return g.at[layer, :, lo:hi] if a < 4 else u.at[layer, :, lo - hidden:hi - hidden] if a < 8 else d.at[layer, :, lo:hi]

    def own_copy(layer, a):
        return pltpu.make_async_copy(own(layer, a, wg_hbm, wu_hbm, wd_hbm), slots[layer][a].at[0], own_sem.at[layer, a])

    def result_copy(layer, a):
        return pltpu.make_async_copy(slots[1][a].at[0], own(layer, a, og_hbm, ou_hbm, od_hbm), own_sem.at[layer, a])

    def exchange(kind, a, rounds, n, source, target):
        before = sum(len(r) for r in rounds[:n])
        return [pltpu.make_async_remote_copy(
            src_ref=source[a].at[pl.ds(here, count)], dst_ref=target[a].at[pl.ds(there, count)],
            send_sem=send_sem.at[kind, a, before + k], recv_sem=recv_sem.at[kind, a, before + k],
            device_id=to(a, slot), device_id_type=MESH) for k, (here, there, count, slot) in enumerate(rounds[n])]

    def gather_copies(layer, n, a):
        return exchange(layer, a, GATHER, n, slots[layer], slots[layer])

    def hand_copy(layer, n, a):
        there = slots[layer][a].at[pl.ds(*((1, 3), (4, 4), (8, 8))[n])]
        return pltpu.make_async_remote_copy(
            src_ref=there, dst_ref=there, send_sem=hand_send.at[layer, a, n], recv_sem=hand_recv.at[layer, a, n],
            device_id=partner, device_id_type=MESH)

    def by_core(arrays, act):
        for side in range(2):
            @pl.when(core == side)
            def _():
                act([a for a in arrays if keeper[a] == side], [a for a in arrays if keeper[a] != side])

    def gather_step(layer, n, arrays):
        def act(mine, _):
            for a in mine:
                if n > 0:
                    wait(gather_copies(layer, n - 1, a))
                if n < ROUNDS:
                    start(gather_copies(layer, n, a))
                if n > 0:
                    hand_copy(layer, n - 1, a).start()
        by_core(arrays, act)

    def gather_end(layer, arrays):
        def act(mine, others):
            for n in range(ROUNDS):
                for a in others:
                    hand_copy(layer, n, a).wait_recv()
                for a in mine:
                    hand_copy(layer, n, a).wait_send()
        by_core(arrays, act)

    def install(layer, arrays):
        for r in range(16):
            for a in arrays:
                lo, hi = cols[a]
                if a < 8:
                    wgu[layer, rows_of(a, r), lo:hi] = slots[layer][a][r]
                else:
                    acc_d[layer, rows_of(a, r), lo:hi] = slots[layer][a][r].astype(f32)

    def scatter_copies(layer, n, a):
        return exchange(2 + layer, a, SCATTER, n, slots[1], slots[0])

    def scatter_start(layer, n, arrays):
        for a in arrays:
            before = sum(len(r) for r in SCATTER[:n])
            for k, copy in enumerate(scatter_copies(layer, n, a)):
                if layer == 0:
                    pl.semaphore_wait(credit.at[a, before + k], 1)
                copy.start()

    def scatter_fill(layer, arrays):
        for a in arrays:
            lo, hi = cols[a]
            acc = acc_gu if a < 8 else acc_d
            for r in range(8, 16):
                slots[1][a][r] = acc[layer, rows_of(a, r), lo:hi].astype(bf16)
        scatter_start(layer, 0, arrays)

    def scatter_add(layer, n, arrays):
        keep, stay = ((8, 4), (4, 1), (1, 0))[n]
        for a in arrays:
            lo, hi = cols[a]
            acc = acc_gu if a < 8 else acc_d
            wait(scatter_copies(layer, n, a))
            for r in reversed(range(keep)):
                total = acc[layer, rows_of(a, r), lo:hi]
                for _, there, count, _ in SCATTER[n]:
                    if r < count:
                        total += slots[0][a][there + r].astype(f32)
                if n == ROUNDS - 1:
                    if layer == 0:
                        result_copy(1, a).wait()
                    slots[1][a][0] = total.astype(bf16)
                    result_copy(layer, a).start()
                elif r >= stay:
                    slots[1][a][r] = total.astype(bf16)
                else:
                    acc[layer, rows_of(a, r), lo:hi] = total
            if layer == 1:
                before = sum(len(r) for r in SCATTER[:n])
                for k, (_, _, _, slot) in enumerate(SCATTER[n]):
                    pl.semaphore_signal(credit.at[a, before + k], inc=1, device_id=to(a, slot), device_id_type=MESH)
        if n < ROUNDS - 1:
            scatter_start(layer, n + 1, arrays)

    def chunks_of(lo, hi):
        return [(at, min(at + CHUNK, hi)) for at in range(lo, hi, CHUNK)]

    def normed(h):
        wide = h.astype(f32)
        scale = lax.rsqrt(jnp.mean(wide * wide, -1, keepdims=True) + 1e-6)
        return wide, scale, (wide * scale).astype(bf16)

    def loop(events, body, n=tiles):
        def step(i, _):
            for when, actions in events.items():
                @pl.when(i == when)
                def _():
                    for act, *args in actions:
                        act(*args)
            body(i)
            return 0
        lax.fori_loop(0, n, step, 0)

    def transposes(layer, down):
        for lo in range(0, 2 * hidden, CHUNK):
            wgut[lo:lo + CHUNK, :] = wgu[layer, :, lo:lo + CHUNK].T
        for lo, hi, block in down:
            wdt[:, lo:hi] = block[...].T.astype(bf16)

    def inner(g, u, dq):
        dq = dq.astype(bf16).astype(f32)
        sig = 0.5 * jnp.tanh(0.5 * g) + 0.5
        s = g * sig
        return (s * u).astype(bf16), (dq * u * (sig + s * (1 - sig))).astype(bf16), (dq * s).astype(bf16)

    def outer(wide, scale, dy, da):
        da = da.astype(bf16).astype(f32)
        mean = jnp.mean(da * wide, -1, keepdims=True)
        return dy + (da * scale - wide * (mean * scale * scale * scale)).astype(bf16)

    every = range(12)
    for layer in range(2):
        start([own_copy(layer, a) for a in every])
    in_copy(x_hbm, 0).start()
    barrier = pltpu.get_barrier_semaphore()
    peers = [to(a, slot) for a in range(8, 12) for slot in (1, 3)]
    for peer in peers + [partner]:
        pl.semaphore_signal(barrier, inc=1, device_id=peer, device_id_type=MESH)
    wait([own_copy(0, a) for a in every])
    pl.semaphore_wait(barrier, 9)
    for n in range(ROUNDS):
        gather_step(0, n, GU)
        gather_step(0, n, D)
    wait([own_copy(1, a) for a in every])
    gather_step(1, 0, every)
    in_copy(x_hbm, 0).wait()
    a_s[0] = normed(in_s[0])[2]
    gather_step(0, ROUNDS, GU)
    gather_end(0, GU)
    install(0, GU)

    def p_out(i):
        return pltpu.make_async_copy(p_s.at[lax.rem(i, 2)], p_hbm.at[at_tile(i)], p_sem.at[lax.rem(i, 2)])

    def gu_out(i):
        return pltpu.make_async_copy(acc_gu.at[lax.rem(i, 2)], gu_hbm.at[at_tile(i)], gu_sem.at[lax.rem(i, 2), 0])

    def a_out(i):
        return pltpu.make_async_copy(a_s.at[lax.rem(i, 2)], a_hbm.at[at_tile(i)], a_sem.at[lax.rem(i, 2)])

    def next_x(i):
        slot = lax.rem(i + 1, 2)
        return pltpu.make_async_copy(x_hbm.at[at_tile(jnp.minimum(i + 1, tiles - 1))], in_s.at[slot], in_sem.at[slot])

    def down(slot):
        return sum(dot(p_s[slot, :, lo:hi], block[...]) for lo, hi, block in wd0).astype(bf16)

    def forward(i):
        slot = lax.rem(i, 2)
        next_x(i).start()
        a_out(i).start()

        @pl.when(i >= 1)
        def _():
            a_out(i - 1).wait()

        @pl.when(i >= 2)
        def _():
            p_out(i - 2).wait()
            gu_out(i - 2).wait()

        @pl.when(i == 1)
        def _():
            gather_step(0, ROUNDS, D)
            gather_end(0, D)
            install(0, D)
            for lo, hi, block in wd0:
                block[...] = acc_d[0, lo:hi].astype(bf16)
            for peer in peers:
                pl.semaphore_signal(ready, inc=1, device_id=peer, device_id_type=MESH)
        before = at_tile(jnp.maximum(i - 1, 0))
        h_s[before, :] += down(1 - slot)
        h_s[at_tile(i), :] = in_s[slot]
        a = a_s[slot]
        for lo, hi in chunks_of(0, hidden):
            g, u = dot(a, wgu[0, :, lo:hi]), dot(a, wgu[0, :, hidden + lo:hidden + hi])
            sig = 0.5 * jnp.tanh(0.5 * g) + 0.5
            s = g * sig
            p_s[slot, :, lo:hi] = (s * u).astype(bf16)
            acc_gu[slot, :, lo:hi] = u * (sig + s * (1 - sig))
            acc_gu[slot, :, hidden + lo:hidden + hi] = s
        p_out(i).start()
        gu_out(i).start()
        next_x(i).wait()
        a_s[1 - slot] = normed(in_s[1 - slot])[2]

    loop({1: [(gather_step, 1, 1, every)], 3: [(gather_step, 1, 2, every)], 7: [(gather_step, 1, ROUNDS, every)]}, forward)
    h_s[at_tile(tiles - 1), :] += down((tiles - 1) % 2)
    a_out(tiles - 1).wait()
    in_copy(dy_hbm, 0).start()
    gather_end(1, every)
    install(1, every)
    transposes(1, [(lo, hi, acc_d.at[1, lo:hi]) for lo, hi in chunks_of(0, hidden)])
    acc_d[...] = jnp.zeros_like(acc_d)
    for i in (tiles - 2, tiles - 1):
        p_out(i).wait()
        gu_out(i).wait()
    acc_gu[...] = jnp.zeros_like(acc_gu)

    first, second = (0, half), (half, hidden)

    def gu_in(i, span):
        slot, n = lax.rem(i, 2), span[1] - span[0]
        return [pltpu.make_async_copy(gu_hbm.at[at_tile(i), pl.ds(side * hidden + span[0], n)], gu_s.at[slot, :, pl.ds(side * half, n)],
                                      gu_sem.at[slot, side]) for side in range(2)]

    def p_in(i):
        return pltpu.make_async_copy(p_hbm.at[at_tile(i)], p_s.at[lax.rem(i, 2)], p_sem.at[lax.rem(i, 2)])

    def last(i):
        rows = at_tile(i)
        wide, scale, a = normed(h_s[rows, :])
        dy = streamed(dy_hbm, a_hbm, i)
        for lo, hi in chunks_of(0, hidden):
            g, u = dot(a, wgu[1, :, lo:hi]), dot(a, wgu[1, :, hidden + lo:hidden + hi])
            p_s[0, :, lo:hi], dgu_s[0, :, lo:hi], dgu_s[0, :, hidden + lo:hidden + hi] = inner(g, u, dot(dy, wdt[:, lo:hi]))
        h_s[rows, :] = outer(wide, scale, dy, dot(dgu_s[0], wgut[...]))
        acc_d[1] += dot_t(p_s[0], dy)
        acc_gu[1] += dot_t(a, dgu_s[0])

    start(gu_in(0, first))
    loop({}, last)
    p_in(0).start()
    pl.semaphore_wait(ready, len(peers))
    for arrays in (FIRST, SECOND, D):
        scatter_fill(1, arrays)
    transposes(0, [(lo, min(lo + CHUNK, hi), block.at[lo - begin:min(lo + CHUNK, hi) - begin]) for begin, hi, block in wd0 for lo in range(begin, hi, CHUNK)])

    def dgu_copies(i, span, out):
        slot = lax.rem(i, 2)
        found = []
        for side in range(2):
            place = pl.ds(side * hidden + span[0], span[1] - span[0])
            there, here = dgu_hbm.at[at_tile(i), place], dgu_s.at[slot, :, place]
            found.append(pltpu.make_async_copy(*((here, there) if out else (there, here)), dgu_sem.at[slot, side, int(out)]))
        return found

    def gate_up(i, span, following, after, down=False):
        slot = lax.rem(i, 2)
        dy = h_s[at_tile(i), :]
        a = streamed(a_hbm, following, i)
        if down:
            @pl.when(i < tiles - 1)
            def _():
                p_in(i + 1).start()
            p_in(i).wait()

        @pl.when(i < tiles - 1)
        def _():
            start(gu_in(i + 1, span))

        @pl.when(i == tiles - 1)
        def _():
            after()

        @pl.when(i >= 2)
        def _():
            wait(dgu_copies(i - 2, span, True))
        wait(gu_in(i, span))
        if down:
            acc_d[0] += dot_t(p_s[slot], dy)
        for lo, hi in chunks_of(*span):
            here = [slice(at + lo - span[0], at + hi - span[0]) for at in (0, half)]
            dq = dot(dy, wdt[:, lo:hi]).astype(bf16).astype(f32)
            dgu_s[slot, :, lo:hi] = (dq * gu_s[slot, :, here[0]]).astype(bf16)
            dgu_s[slot, :, hidden + lo:hidden + hi] = (dq * gu_s[slot, :, here[1]]).astype(bf16)
        for side in range(2):
            lo, hi = (side * hidden + at for at in span)
            acc_gu[0, :, lo:hi] += dot_t(a, dgu_s[slot, :, lo:hi])
        start(dgu_copies(i, span, True))

    def drain(span):
        for i in range(tiles - 2, tiles):
            wait(dgu_copies(i, span, True))

    whole, da_s = (0, hidden), gu_s.at[0, :, :width]

    def x_in(i):
        tile = tiles - 1 - i
        return pltpu.make_async_copy(x_hbm.at[at_tile(tile)], in_s.at[lax.rem(i, 2)], in_sem.at[lax.rem(i, 2)])

    def dgu_in(i):
        return dgu_copies(tiles - 1 - i, whole, False)

    def dx_out(i):
        rows = at_tile(tiles - 1 - i)
        return pltpu.make_async_copy(h_s.at[rows], dx_hbm.at[rows], dx_sem.at[i])

    def back(i):
        rows = at_tile(tiles - 1 - i)
        if isinstance(i, int):
            x_in(i).wait()
            ahead = i < tiles - 1
        else:
            @pl.when(i < tiles - 2)
            def _():
                start(dgu_in(i + 2))

            @pl.when(i >= 1)
            def _():
                wait(dgu_in(i + 1))
            x_in(i + 1).start()
            x_in(i).wait()
            ahead = True
        wide, scale, _ = normed(in_s[i % 2 if isinstance(i, int) else lax.rem(i, 2)])
        h_s[rows, :] = outer(wide, scale, h_s[rows, :], da_s[...])
        dx_out(i).start()
        if ahead:
            da_s[...] = dot(dgu_s[lax.rem(tiles - 2 - i, 2)], wgut[...])

    loop({3: [(scatter_add, 1, 0, FIRST)], 5: [(scatter_add, 1, 0, SECOND)], 6: [(scatter_add, 1, 0, D)], 7: [(scatter_add, 1, 1, FIRST)]},
         lambda i: gate_up(i, first, a_hbm, lambda: start(gu_in(0, second)), True))
    scatter_add(1, 1, SECOND)
    scatter_fill(0, D)
    drain(first)
    scatter_fill(0, FIRST)
    loop({1: [(scatter_add, 1, 1, D)], 3: [(scatter_add, 1, 2, FIRST)], 4: [(scatter_add, 1, 2, SECOND)], 5: [(scatter_add, 0, 0, D)],
          7: [(scatter_add, 0, 0, FIRST)]}, lambda i: gate_up(i, second, None, lambda: x_in(0).start()))
    drain(second)
    scatter_fill(0, SECOND)
    scatter_add(1, 2, D)
    da_s[...] = dot(dgu_s[(tiles - 1) % 2], wgut[...])
    loop({1: [(scatter_add, 0, 1, D)], 2: [(scatter_add, 0, 0, SECOND), (scatter_add, 0, 1, FIRST)], 4: [(scatter_add, 0, 2, D)],
          5: [(scatter_add, 0, 1, SECOND), (scatter_add, 0, 2, FIRST)]}, back, tiles - 1)
    back(tiles - 1)
    scatter_add(0, 2, SECOND)
    wait([dx_out(i) for i in range(tiles)])
    wait([result_copy(0, a) for a in every])


def hand_over(*refs):
    n = len(refs) // 4
    sources, targets, held, sems = refs[:n], refs[n:2 * n], refs[2 * n:3 * n], refs[3 * n:]
    pairs = []
    for k in range(n):
        rows = sources[k].shape[0] // sems[k].shape[1]
        for i in range(sems[k].shape[1]):
            at = pl.ds(i * rows, rows)
            pairs.append((pltpu.make_async_copy(sources[k].at[at], held[k].at[at], sems[k].at[0, i]),
                          pltpu.make_async_copy(held[k].at[at], targets[k].at[at], sems[k].at[1, i])))
    for into, _ in pairs:
        into.start()
    for into, out in pairs:
        into.wait()
        out.start()
    for _, out in pairs:
        out.wait()


def pieces_of(hidden):
    lanes = hidden // 128
    cuts = [128 * -(-lanes * q // 4) for q in range(5)]
    return list(zip(cuts, cuts[1:]))


def solution(mesh):
    group = mesh.shape["dp"]
    side = math.isqrt(group)
    assert side * side == group == 2**STEPS

    def local(x, dy, w_gate, w_up, w_down):
        _, tokens, width = x.shape
        layers, share_gu, hidden = w_gate.shape
        share_d = w_down.shape[1]
        parts = [pltpu.VMEM((group, share_gu, hi - lo), bf16) for lo, hi in pieces_of(hidden) * 2]
        parts += [pltpu.VMEM((group, share_d, width // 4), bf16)] * 4
        any_, vmem = pl.BlockSpec(memory_space=pl.ANY), pl.BlockSpec(memory_space=pltpu.VMEM)
        shapes = ((tokens, width), w_gate.shape, w_up.shape, w_down.shape, (tokens, hidden), (tokens, 2 * hidden), (tokens, width))
        dma = pltpu.SemaphoreType.DMA
        out = pl.pallas_call(
            functools.partial(kernel, (tokens, width, hidden, share_gu, share_d)),
            out_shape=[jax.ShapeDtypeStruct(s, bf16) for s in shapes] + [jax.ShapeDtypeStruct((tokens, 2 * hidden), f32)],
            in_specs=[any_] * 5,
            out_specs=[any_] * 8,
            scratch_shapes=[
                pltpu.VMEM((2, TILE, width), bf16),
                pltpu.VMEM((tokens, width), bf16),
                pltpu.VMEM((2, TILE, 2 * pieces_of(hidden)[2][0]), f32),
                pltpu.VMEM((layers, width, 2 * hidden), bf16),
                pltpu.VMEM((2 * hidden, width), bf16),
                pltpu.VMEM((width, hidden), bf16),
                pltpu.VMEM((layers, width, 2 * hidden), f32),
                pltpu.VMEM((layers, hidden, width), f32),
                pltpu.VMEM((2, TILE, hidden), bf16),
                pltpu.VMEM((2, TILE, 2 * hidden), bf16),
            ] + parts * 2 + [
                dma((4, 12, 5)), dma((4, 12, 5)), dma((2, 12, ROUNDS)), dma((2, 12, ROUNDS)),
                pltpu.SemaphoreType.REGULAR((12, 5)), dma((2, 12)), dma((2,)), dma((2,)), dma((2,)), dma((2, 2, 2)), dma((2, 2)), dma((tokens // TILE,)),
                pltpu.SemaphoreType.REGULAR,
            ],
            compiler_params=pltpu.CompilerParams(collective_id=0, has_side_effects=True, vmem_limit_bytes=VMEM_LIMIT),
            name="stack",
        )(x[0], dy[0], w_gate, w_up, w_down)
        shapes = [t.shape for t in out[:4]]
        results = pl.pallas_call(
            hand_over,
            out_shape=[jax.ShapeDtypeStruct(s, bf16) for s in shapes],
            in_specs=[any_] * 4,
            out_specs=[any_] * 4,
            scratch_shapes=[pltpu.VMEM(s, bf16) for s in shapes] + [dma((2, n)) for n in (8, 1, 1, 1)],
            name="hand_over",
        )(*out[:4])
        return (results[0][None], *results[1:])

    tokens_spec = P(("rep", "dp"), None, None)
    weight_spec, grad_spec = P(None, "dp", None), P("rep", "dp", None)
    return jax.shard_map(local, mesh=mesh, in_specs=(tokens_spec, tokens_spec) + (weight_spec,) * 3,
                         out_specs=(tokens_spec,) + (grad_spec,) * 3, check_vma=False)
```

```python
import functools
import math

import jax
import jax.numpy as jnp
from jax import lax
from jax.experimental import pallas as pl
from jax.experimental.pallas import tpu as pltpu
from jax.sharding import PartitionSpec as P

bf16, f32 = jnp.bfloat16, jnp.float32
MESH = pl.DeviceIdType.MESH
TILE = 512
CHUNK = 256
STEPS = 4
GATHER = (((0, 1, 1, 1), (0, 2, 1, 2), (0, 3, 1, 3)), ((0, 4, 4, 4),), ((0, 8, 8, 8),))
SCATTER = (((8, 8, 8, 8),), ((4, 4, 4, 4),), ((1, 1, 1, 1), (2, 2, 1, 2), (3, 3, 1, 3)))
ROUNDS = 3
VMEM_LIMIT = 67043328
DIMS = ((1, 0), (0, 1), (3, 0), (0, 3))
PART = (0, 1, 0, 1, 2, 3, 2, 3, 0, 1, 2, 3)


def dot(a, b):
    return jnp.dot(a, b, preferred_element_type=f32)


def dot_t(a, b):
    return lax.dot_general(a, b, (((0,), (0,)), ((), ())), preferred_element_type=f32)


def flip(c, bits):
    return (c, c + 1 - 2 * lax.rem(c, 2), lax.rem(c + 2, 4), 3 - c)[bits]


def mask_of(part, slot):
    x = y = 0
    for bit in range(STEPS):
        if slot >> bit & 1:
            dx, dy = DIMS[(part + STEPS - 1 - bit) % 4]
            x, y = x ^ dx, y ^ dy
    return x, y


def kernel(sizes, x_hbm, dy_hbm, wg_hbm, wu_hbm, wd_hbm, dx_hbm, og_hbm, ou_hbm, od_hbm, p_hbm, dgu_hbm, a_hbm, gu_hbm, *scratch):
    (in_s, h_s, gu_s, wgu, wgut, wdt, acc_gu, acc_d, p_s, dgu_s, tail, *rest) = scratch
    slots = (rest[:12], rest[12:24])
    send_sem, recv_sem, hand_send, hand_recv, credit, own_sem, in_sem, a_sem, p_sem, dgu_sem, gu_sem, dx_sem, ready = rest[24:]
    tokens, width, hidden, share_gu, share_d = sizes
    a_s = dgu_s.at[:, :, :width]
    wd0 = [(lo, min(lo + TILE, hidden), dgu_s.at[1, :min(TILE, hidden - lo), pl.ds((1 + lo // TILE) * width, width)]) for lo in range(0, hidden, TILE)]
    me, rep = lax.axis_index("dp"), lax.axis_index("rep")
    mx, my = lax.div(me, 4), lax.rem(me, 4)
    core = lax.rem(rep, 2)
    tiles = tokens // TILE

    def device(mask):
        return flip(mx, mask[0]) * 4 + flip(my, mask[1])

    def to(a, slot):
        return {"dp": device(mask_of(PART[a], slot))}

    partner = {"rep": rep + 1 - 2 * core}
    pieces = pieces_of(hidden)
    cols = pieces + [(hidden + lo, hidden + hi) for lo, hi in pieces] + [(width * q // 4, width * (q + 1) // 4) for q in range(4)]
    GU, D = range(8), range(8, 12)
    half = pieces[2][0]
    FIRST, SECOND = (0, 1, 4, 5), (2, 3, 6, 7)
    keeper = (0, 0, 0, 0, 1, 1, 1, 1, 0, 0, 1, 1)

    def in_copy(source, i):
        return pltpu.make_async_copy(source.at[at_tile(i)], in_s.at[lax.rem(i, 2)], in_sem.at[lax.rem(i, 2)])

    def streamed(source, following, i):
        @pl.when(i < tiles - 1)
        def _():
            in_copy(source, i + 1).start()
        if following is not None:
            @pl.when(i == tiles - 1)
            def _():
                in_copy(following, 0).start()
        in_copy(source, i).wait()
        return in_s[lax.rem(i, 2)]

    def at_tile(i):
        if isinstance(i, int):
            return pl.ds(i * TILE, TILE)
        return pl.ds(pl.multiple_of(i * TILE, TILE), TILE)

    def start(copies):
        for copy in copies:
            copy.start()

    def wait(copies):
        for copy in copies:
            copy.wait()

    def rows_of(a, slot):
        share = share_gu if a < 8 else share_d
        return pl.ds(pl.multiple_of(device(mask_of(PART[a], slot)) * share, 8), share)

    def own(layer, a, g, u, d):
        lo, hi = cols[a]
        return g.at[layer, :, lo:hi] if a < 4 else u.at[layer, :, lo - hidden:hi - hidden] if a < 8 else d.at[layer, :, lo:hi]

    def own_copy(layer, a):
        return pltpu.make_async_copy(own(layer, a, wg_hbm, wu_hbm, wd_hbm), slots[layer][a].at[0], own_sem.at[layer, a])

    def result_copy(layer, a):
        return pltpu.make_async_copy(slots[1][a].at[0], own(layer, a, og_hbm, ou_hbm, od_hbm), own_sem.at[layer, a])

    def exchange(kind, a, rounds, n, source, target):
        before = sum(len(r) for r in rounds[:n])
        return [pltpu.make_async_remote_copy(
            src_ref=source[a].at[pl.ds(here, count)], dst_ref=target[a].at[pl.ds(there, count)],
            send_sem=send_sem.at[kind, a, before + k], recv_sem=recv_sem.at[kind, a, before + k],
            device_id=to(a, slot), device_id_type=MESH) for k, (here, there, count, slot) in enumerate(rounds[n])]

    def gather_copies(layer, n, a):
        return exchange(layer, a, GATHER, n, slots[layer], slots[layer])

    def hand_copy(layer, n, a):
        there = slots[layer][a].at[pl.ds(*((1, 3), (4, 4), (8, 8))[n])]
        return pltpu.make_async_remote_copy(
            src_ref=there, dst_ref=there, send_sem=hand_send.at[layer, a, n], recv_sem=hand_recv.at[layer, a, n],
            device_id=partner, device_id_type=MESH)

    def by_core(arrays, act):
        for side in range(2):
            @pl.when(core == side)
            def _():
                act([a for a in arrays if keeper[a] == side], [a for a in arrays if keeper[a] != side])

    def gather_step(layer, n, arrays):
        def act(mine, _):
            for a in mine:
                if n > 0:
                    wait(gather_copies(layer, n - 1, a))
                if n < ROUNDS:
                    start(gather_copies(layer, n, a))
                if n > 0:
                    hand_copy(layer, n - 1, a).start()
        by_core(arrays, act)

    def gather_end(layer, arrays):
        def act(mine, others):
            for n in range(ROUNDS):
                for a in others:
                    hand_copy(layer, n, a).wait_recv()
                for a in mine:
                    hand_copy(layer, n, a).wait_send()
        by_core(arrays, act)

    def install(layer, arrays):
        for r in range(16):
            for a in arrays:
                lo, hi = cols[a]
                if a < 8:
                    wgu[layer, rows_of(a, r), lo:hi] = slots[layer][a][r]
                else:
                    acc_d[layer, rows_of(a, r), lo:hi] = slots[layer][a][r].astype(f32)

    def scatter_copies(layer, n, a):
        return exchange(2 + layer, a, SCATTER, n, slots[1], slots[0])

    def scatter_start(layer, n, arrays):
        for a in arrays:
            before = sum(len(r) for r in SCATTER[:n])
            for k, copy in enumerate(scatter_copies(layer, n, a)):
                if layer == 0:
                    pl.semaphore_wait(credit.at[a, before + k], 1)
                copy.start()

    def scatter_fill(layer, arrays):
        for a in arrays:
            lo, hi = cols[a]
            acc = acc_gu if a < 8 else acc_d
            for r in range(8, 16):
                slots[1][a][r] = acc[layer, rows_of(a, r), lo:hi].astype(bf16)
        scatter_start(layer, 0, arrays)

    def scatter_add(layer, n, arrays):
        keep, stay = ((8, 4), (4, 1), (1, 0))[n]
        for a in arrays:
            lo, hi = cols[a]
            acc = acc_gu if a < 8 else acc_d
            wait(scatter_copies(layer, n, a))
            for r in reversed(range(keep)):
                total = acc[layer, rows_of(a, r), lo:hi]
                for _, there, count, _ in SCATTER[n]:
                    if r < count:
                        total += slots[0][a][there + r].astype(f32)
                if n == ROUNDS - 1:
                    if layer == 0:
                        result_copy(1, a).wait()
                    slots[1][a][0] = total.astype(bf16)
                    result_copy(layer, a).start()
                elif r >= stay:
                    slots[1][a][r] = total.astype(bf16)
                else:
                    acc[layer, rows_of(a, r), lo:hi] = total
            if layer == 1:
                before = sum(len(r) for r in SCATTER[:n])
                for k, (_, _, _, slot) in enumerate(SCATTER[n]):
                    pl.semaphore_signal(credit.at[a, before + k], inc=1, device_id=to(a, slot), device_id_type=MESH)
        if n < ROUNDS - 1:
            scatter_start(layer, n + 1, arrays)

    def chunks_of(lo, hi):
        return [(at, min(at + CHUNK, hi)) for at in range(lo, hi, CHUNK)]

    def normed(h):
        wide = h.astype(f32)
        scale = lax.rsqrt(jnp.mean(wide * wide, -1, keepdims=True) + 1e-6)
        return wide, scale, (wide * scale).astype(bf16)

    def tails(layer):
        n = hidden % CHUNK
        tail[layer, :, :n] = wgu[layer, :, hidden - n:hidden]
        tail[layer, :, n:] = wgu[layer, :, 2 * hidden - n:]

    def project(layer, a, lo, hi):
        if hi - lo == CHUNK:
            return dot(a, wgu[layer, :, lo:hi]), dot(a, wgu[layer, :, hidden + lo:hidden + hi])
        both = dot(a, tail[layer])
        return both[:, :hi - lo], both[:, hi - lo:]

    def loop(events, body, n=tiles):
        def step(i, _):
            for when, actions in events.items():
                @pl.when(i == when)
                def _():
                    for act, *args in actions:
                        act(*args)
            body(i)
            return 0
        lax.fori_loop(0, n, step, 0)

    def transposes(layer, down):
        for lo in range(0, 2 * hidden, CHUNK):
            wgut[lo:lo + CHUNK, :] = wgu[layer, :, lo:lo + CHUNK].T
        for lo, hi, block in down:
            wdt[:, lo:hi] = block[...].T.astype(bf16)

    def inner(g, u, dq):
        dq = dq.astype(bf16).astype(f32)
        sig = 0.5 * jnp.tanh(0.5 * g) + 0.5
        s = g * sig
        return (s * u).astype(bf16), (dq * u * (sig + s * (1 - sig))).astype(bf16), (dq * s).astype(bf16)

    def outer(wide, scale, dy, da):
        da = da.astype(bf16).astype(f32)
        mean = jnp.mean(da * wide, -1, keepdims=True)
        return dy + (da * scale - wide * (mean * scale * scale * scale)).astype(bf16)

    every = range(12)
    for layer in range(2):
        start([own_copy(layer, a) for a in every])
    in_copy(x_hbm, 0).start()
    barrier = pltpu.get_barrier_semaphore()
    peers = [to(a, slot) for a in range(8, 12) for slot in (1, 3)]
    for peer in peers + [partner]:
        pl.semaphore_signal(barrier, inc=1, device_id=peer, device_id_type=MESH)
    wait([own_copy(0, a) for a in every])
    pl.semaphore_wait(barrier, 9)
    for n in range(ROUNDS):
        gather_step(0, n, GU)
        gather_step(0, n, D)
    wait([own_copy(1, a) for a in every])
    gather_step(1, 0, every)
    in_copy(x_hbm, 0).wait()
    a_s[0] = normed(in_s[0])[2]
    gather_step(0, ROUNDS, GU)
    gather_end(0, GU)
    install(0, GU)
    tails(0)

    def p_out(i):
        return pltpu.make_async_copy(p_s.at[lax.rem(i, 2)], p_hbm.at[at_tile(i)], p_sem.at[lax.rem(i, 2)])

    def gu_out(i):
        return pltpu.make_async_copy(acc_gu.at[lax.rem(i, 2)], gu_hbm.at[at_tile(i)], gu_sem.at[lax.rem(i, 2), 0])

    def a_out(i):
        return pltpu.make_async_copy(a_s.at[lax.rem(i, 2)], a_hbm.at[at_tile(i)], a_sem.at[lax.rem(i, 2)])

    def next_x(i):
        slot = lax.rem(i + 1, 2)
        return pltpu.make_async_copy(x_hbm.at[at_tile(jnp.minimum(i + 1, tiles - 1))], in_s.at[slot], in_sem.at[slot])

    def down(slot):
        return sum(dot(p_s[slot, :, lo:hi], block[...]) for lo, hi, block in wd0).astype(bf16)

    def forward(i):
        slot = lax.rem(i, 2)
        next_x(i).start()
        a_out(i).start()

        @pl.when(i >= 1)
        def _():
            a_out(i - 1).wait()

        @pl.when(i >= 2)
        def _():
            p_out(i - 2).wait()
            gu_out(i - 2).wait()

        @pl.when(i == 1)
        def _():
            gather_step(0, ROUNDS, D)
            gather_end(0, D)
            install(0, D)
            for lo, hi, block in wd0:
                block[...] = acc_d[0, lo:hi].astype(bf16)
            for peer in peers:
                pl.semaphore_signal(ready, inc=1, device_id=peer, device_id_type=MESH)
        before = at_tile(jnp.maximum(i - 1, 0))
        h_s[before, :] += down(1 - slot)
        h_s[at_tile(i), :] = in_s[slot]
        a = a_s[slot]
        for lo, hi in chunks_of(0, hidden):
            g, u = project(0, a, lo, hi)
            sig = 0.5 * jnp.tanh(0.5 * g) + 0.5
            s = g * sig
            p_s[slot, :, lo:hi] = (s * u).astype(bf16)
            acc_gu[slot, :, lo:hi] = u * (sig + s * (1 - sig))
            acc_gu[slot, :, hidden + lo:hidden + hi] = s
        p_out(i).start()
        gu_out(i).start()
        next_x(i).wait()
        a_s[1 - slot] = normed(in_s[1 - slot])[2]

    loop({1: [(gather_step, 1, 1, every)], 3: [(gather_step, 1, 2, every)], 7: [(gather_step, 1, ROUNDS, every)]}, forward)
    h_s[at_tile(tiles - 1), :] += down((tiles - 1) % 2)
    a_out(tiles - 1).wait()
    in_copy(dy_hbm, 0).start()
    gather_end(1, every)
    install(1, every)
    tails(1)
    transposes(1, [(lo, hi, acc_d.at[1, lo:hi]) for lo, hi in chunks_of(0, hidden)])
    acc_d[...] = jnp.zeros_like(acc_d)
    for i in (tiles - 2, tiles - 1):
        p_out(i).wait()
        gu_out(i).wait()
    acc_gu[...] = jnp.zeros_like(acc_gu)

    first, second = (0, half), (half, hidden)

    def gu_in(i, span):
        slot, n = lax.rem(i, 2), span[1] - span[0]
        return [pltpu.make_async_copy(gu_hbm.at[at_tile(i), pl.ds(side * hidden + span[0], n)], gu_s.at[slot, :, pl.ds(side * half, n)],
                                      gu_sem.at[slot, side]) for side in range(2)]

    def p_in(i):
        return pltpu.make_async_copy(p_hbm.at[at_tile(i)], p_s.at[lax.rem(i, 2)], p_sem.at[lax.rem(i, 2)])

    def last(i):
        rows = at_tile(i)
        wide, scale, a = normed(h_s[rows, :])
        dy = streamed(dy_hbm, a_hbm, i)
        for lo, hi in chunks_of(0, hidden):
            g, u = project(1, a, lo, hi)
            p_s[0, :, lo:hi], dgu_s[0, :, lo:hi], dgu_s[0, :, hidden + lo:hidden + hi] = inner(g, u, dot(dy, wdt[:, lo:hi]))
        h_s[rows, :] = outer(wide, scale, dy, dot(dgu_s[0], wgut[...]))
        acc_d[1] += dot_t(p_s[0], dy)
        acc_gu[1] += dot_t(a, dgu_s[0])

    for i in range(2):
        start(gu_in(i, first))
    loop({}, last)
    p_in(0).start()
    pl.semaphore_wait(ready, len(peers))
    for arrays in (FIRST, SECOND, D):
        scatter_fill(1, arrays)
    transposes(0, [(lo, min(lo + CHUNK, hi), block.at[lo - begin:min(lo + CHUNK, hi) - begin]) for begin, hi, block in wd0 for lo in range(begin, hi, CHUNK)])

    def dgu_copies(i, span, out):
        slot = lax.rem(i, 2)
        found = []
        for side in range(2):
            place = pl.ds(side * hidden + span[0], span[1] - span[0])
            there, here = dgu_hbm.at[at_tile(i), place], dgu_s.at[slot, :, place]
            found.append(pltpu.make_async_copy(*((here, there) if out else (there, here)), dgu_sem.at[slot, side, int(out)]))
        return found

    def gate_up(i, span, following, after, down=False):
        slot = lax.rem(i, 2)
        dy = h_s[at_tile(i), :]
        a = streamed(a_hbm, following, i)
        if down:
            @pl.when(i < tiles - 1)
            def _():
                p_in(i + 1).start()
            p_in(i).wait()

        @pl.when(i >= 2)
        def _():
            wait(dgu_copies(i - 2, span, True))
        wait(gu_in(i, span))
        if down:
            acc_d[0] += dot_t(p_s[slot], dy)
        for lo, hi in chunks_of(*span):
            here = [slice(at + lo - span[0], at + hi - span[0]) for at in (0, half)]
            dq = dot(dy, wdt[:, lo:hi]).astype(bf16).astype(f32)
            dgu_s[slot, :, lo:hi] = (dq * gu_s[slot, :, here[0]]).astype(bf16)
            dgu_s[slot, :, hidden + lo:hidden + hi] = (dq * gu_s[slot, :, here[1]]).astype(bf16)
        for side in range(2):
            lo, hi = (side * hidden + at for at in span)
            acc_gu[0, :, lo:hi] += dot_t(a, dgu_s[slot, :, lo:hi])
        start(dgu_copies(i, span, True))

        @pl.when(i < tiles - 2)
        def _():
            start(gu_in(i + 2, span))

        @pl.when(i >= tiles - 2)
        def _():
            after(i + 2 - tiles)

    def drain(span):
        for i in range(tiles - 2, tiles):
            wait(dgu_copies(i, span, True))

    whole, da_s = (0, hidden), gu_s.at[0, :, :width]

    def x_in(i):
        tile = tiles - 1 - i
        return pltpu.make_async_copy(x_hbm.at[at_tile(tile)], in_s.at[lax.rem(i, 2)], in_sem.at[lax.rem(i, 2)])

    def dgu_in(i):
        return dgu_copies(tiles - 1 - i, whole, False)

    def dx_out(i):
        rows = at_tile(tiles - 1 - i)
        return pltpu.make_async_copy(h_s.at[rows], dx_hbm.at[rows], dx_sem.at[i])

    def back(i):
        rows = at_tile(tiles - 1 - i)
        if isinstance(i, int):
            x_in(i).wait()
            ahead = i < tiles - 1
        else:
            @pl.when(i < tiles - 2)
            def _():
                start(dgu_in(i + 2))

            @pl.when(i >= 1)
            def _():
                wait(dgu_in(i + 1))
            x_in(i + 1).start()
            x_in(i).wait()
            ahead = True
        wide, scale, _ = normed(in_s[i % 2 if isinstance(i, int) else lax.rem(i, 2)])
        h_s[rows, :] = outer(wide, scale, h_s[rows, :], da_s[...])
        dx_out(i).start()
        if ahead:
            da_s[...] = dot(dgu_s[lax.rem(tiles - 2 - i, 2)], wgut[...])

    loop({3: [(scatter_add, 1, 0, FIRST)], 5: [(scatter_add, 1, 0, SECOND)], 6: [(scatter_add, 1, 0, D)], 7: [(scatter_add, 1, 1, FIRST)]},
         lambda i: gate_up(i, first, a_hbm, lambda k: start(gu_in(k, second)), True))
    scatter_add(1, 1, SECOND)
    scatter_fill(0, D)
    drain(first)
    scatter_fill(0, FIRST)
    loop({1: [(scatter_add, 1, 1, D)], 3: [(scatter_add, 1, 2, FIRST)], 4: [(scatter_add, 1, 2, SECOND)], 5: [(scatter_add, 0, 0, D)],
          7: [(scatter_add, 0, 0, FIRST)]}, lambda i: gate_up(i, second, None, lambda k: None))
    drain(second)
    x_in(0).start()
    scatter_fill(0, SECOND)
    scatter_add(1, 2, D)
    da_s[...] = dot(dgu_s[(tiles - 1) % 2], wgut[...])
    loop({1: [(scatter_add, 0, 1, D)], 2: [(scatter_add, 0, 0, SECOND), (scatter_add, 0, 1, FIRST)], 4: [(scatter_add, 0, 2, D)],
          5: [(scatter_add, 0, 1, SECOND), (scatter_add, 0, 2, FIRST)]}, back, tiles - 1)
    back(tiles - 1)
    scatter_add(0, 2, SECOND)
    wait([dx_out(i) for i in range(tiles)])
    wait([result_copy(0, a) for a in every])


def hand_over(*refs):
    n = len(refs) // 4
    sources, targets, held, sems = refs[:n], refs[n:2 * n], refs[2 * n:3 * n], refs[3 * n:]
    pairs = []
    for k in range(n):
        rows = sources[k].shape[0] // sems[k].shape[1]
        for i in range(sems[k].shape[1]):
            at = pl.ds(i * rows, rows)
            pairs.append((pltpu.make_async_copy(sources[k].at[at], held[k].at[at], sems[k].at[0, i]),
                          pltpu.make_async_copy(held[k].at[at], targets[k].at[at], sems[k].at[1, i])))
    for into, _ in pairs:
        into.start()
    for into, out in pairs:
        into.wait()
        out.start()
    for _, out in pairs:
        out.wait()


def pieces_of(hidden):
    lanes = hidden // 128
    cuts = [128 * -(-lanes * q // 4) for q in range(5)]
    return list(zip(cuts, cuts[1:]))


def solution(mesh):
    group = mesh.shape["dp"]
    side = math.isqrt(group)
    assert side * side == group == 2**STEPS

    def local(x, dy, w_gate, w_up, w_down):
        _, tokens, width = x.shape
        layers, share_gu, hidden = w_gate.shape
        share_d = w_down.shape[1]
        parts = [pltpu.VMEM((group, share_gu, hi - lo), bf16) for lo, hi in pieces_of(hidden) * 2]
        parts += [pltpu.VMEM((group, share_d, width // 4), bf16)] * 4
        any_, vmem = pl.BlockSpec(memory_space=pl.ANY), pl.BlockSpec(memory_space=pltpu.VMEM)
        shapes = ((tokens, width), w_gate.shape, w_up.shape, w_down.shape, (tokens, hidden), (tokens, 2 * hidden), (tokens, width))
        dma = pltpu.SemaphoreType.DMA
        out = pl.pallas_call(
            functools.partial(kernel, (tokens, width, hidden, share_gu, share_d)),
            out_shape=[jax.ShapeDtypeStruct(s, bf16) for s in shapes] + [jax.ShapeDtypeStruct((tokens, 2 * hidden), f32)],
            in_specs=[any_] * 5,
            out_specs=[any_] * 8,
            scratch_shapes=[
                pltpu.VMEM((2, TILE, width), bf16),
                pltpu.VMEM((tokens, width), bf16),
                pltpu.VMEM((2, TILE, 2 * pieces_of(hidden)[2][0]), f32),
                pltpu.VMEM((layers, width, 2 * hidden), bf16),
                pltpu.VMEM((2 * hidden, width), bf16),
                pltpu.VMEM((width, hidden), bf16),
                pltpu.VMEM((layers, width, 2 * hidden), f32),
                pltpu.VMEM((layers, hidden, width), f32),
                pltpu.VMEM((2, TILE, hidden), bf16),
                pltpu.VMEM((2, TILE, 2 * hidden), bf16),
                pltpu.VMEM((layers, width, 2 * (hidden % CHUNK)), bf16),
            ] + parts * 2 + [
                dma((4, 12, 5)), dma((4, 12, 5)), dma((2, 12, ROUNDS)), dma((2, 12, ROUNDS)),
                pltpu.SemaphoreType.REGULAR((12, 5)), dma((2, 12)), dma((2,)), dma((2,)), dma((2,)), dma((2, 2, 2)), dma((2, 2)), dma((tokens // TILE,)),
                pltpu.SemaphoreType.REGULAR,
            ],
            compiler_params=pltpu.CompilerParams(collective_id=0, has_side_effects=True, vmem_limit_bytes=VMEM_LIMIT),
            name="stack",
        )(x[0], dy[0], w_gate, w_up, w_down)
        shapes = [t.shape for t in out[:4]]
        results = pl.pallas_call(
            hand_over,
            out_shape=[jax.ShapeDtypeStruct(s, bf16) for s in shapes],
            in_specs=[any_] * 4,
            out_specs=[any_] * 4,
            scratch_shapes=[pltpu.VMEM(s, bf16) for s in shapes] + [dma((2, n)) for n in (16, 1, 1, 1)],
            name="hand_over",
        )(*out[:4])
        return (results[0][None], *results[1:])

    tokens_spec = P(("rep", "dp"), None, None)
    weight_spec, grad_spec = P(None, "dp", None), P("rep", "dp", None)
    return jax.shard_map(local, mesh=mesh, in_specs=(tokens_spec, tokens_spec) + (weight_spec,) * 3,
                         out_specs=(tokens_spec,) + (grad_spec,) * 3, check_vma=False)
```
